32 devices in a mesh: site: 4 (over z), py: 2 (over x), px: 2 (over y), pz: 2 (over core).
Axes of the slice: x: 2, y: 2, z: 4, core: 2. Of those that a mesh axis runs over, the one named last changes fastest.
Arguments:
- initial_heat_state: float32 [32, 128, 64, 128], P(('site', 'py'), 'px', 'pz'), parts along dimension 0, may hold values from 0.2 to 1.8
- scaled_speed_north: float32 [32, 128, 64, 128], P(('site', 'py'), 'px', 'pz'), parts along dimension 0, may hold values from -0.3 to 0.3
- scaled_speed_east: float32 [32, 128, 64, 128], P(('site', 'py'), 'px', 'pz'), parts along dimension 0, may hold values from -0.3 to 0.3
- scaled_speed_upward: float32 [32, 128, 64, 128], P(('site', 'py'), 'px', 'pz'), parts along dimension 0, may hold values from -0.3 to 0.3
Outputs:
- temperature_end: float32 [32, 128, 64, 128], P(('site', 'py'), 'px', 'pz'), parts along dimension 0
The draws below stay inside these ranges and needn't reach their ends.
There are 4 independent parts, one for each index of `site`. The reference program is written for one: setup_inputs(seed, part) draws one part's arguments, and reference() takes and returns one part's arrays. A program takes and returns all parts, laid end to end along the dimension named above; each array names one. Nothing has to cross between parts.
All inputs are finite; a program needn't handle non-finite values.
Results may differ from the reference program's by a relative error of at most 0.00002.
Values sent between devices are 32-bit elements; how exact they have to be, the bound alone decides.
A program may use at most 256 MiB of HBM per device.

```python
import jax
import jax.numpy as jnp
from jax import lax

MESH_POINTS_NORTH = 8
MESH_POINTS_EAST = 128
MESH_POINTS_UP = 64
TRACER_TOTAL = 128
STEPS = 4


def block_scale(key, shape, pieces, least, largest):
    gain, own = 1.0, jax.random.fold_in(key, 6)
    for position, blocks in pieces:
        heights = jnp.exp(jax.random.uniform(jax.random.fold_in(own, position), (blocks,), jnp.float32, least / len(pieces), largest / len(pieces)))
        gain = gain * jnp.repeat(heights, shape[position] // blocks).reshape([-1 if axis == position else 1 for axis in range(len(shape))])
    return gain


def setup_inputs(seed: int = 0, part: int = 0) -> dict:
    splits = jax.random.split(jax.random.key(seed), 5)
    part_keys = jax.random.split(jax.random.fold_in(splits[4], part), 5)
    return {
        "initial_heat_state": jnp.clip(0.2 + 1.5999999 * jax.random.uniform(part_keys[0], (MESH_POINTS_NORTH, MESH_POINTS_EAST, MESH_POINTS_UP, TRACER_TOTAL), jnp.float32) ** block_scale(part_keys[0], (MESH_POINTS_NORTH, MESH_POINTS_EAST, MESH_POINTS_UP, TRACER_TOTAL), ((0, 2), (1, 2), (2, 2)), -0.2, 0.2), 0.2, 1.8),
        "scaled_speed_north": jnp.clip(jax.random.uniform(part_keys[1], (MESH_POINTS_NORTH, MESH_POINTS_EAST, MESH_POINTS_UP, TRACER_TOTAL), jnp.float32, -0.3, 0.3) * block_scale(part_keys[1], (MESH_POINTS_NORTH, MESH_POINTS_EAST, MESH_POINTS_UP, TRACER_TOTAL), ((0, 2), (1, 2), (2, 2)), -0.4, 0.0), -0.3, 0.3),
        "scaled_speed_east": jnp.clip(jax.random.uniform(part_keys[2], (MESH_POINTS_NORTH, MESH_POINTS_EAST, MESH_POINTS_UP, TRACER_TOTAL), jnp.float32, -0.3, 0.3) * block_scale(part_keys[2], (MESH_POINTS_NORTH, MESH_POINTS_EAST, MESH_POINTS_UP, TRACER_TOTAL), ((0, 2), (1, 2), (2, 2)), -0.4, 0.0), -0.3, 0.3),
        "scaled_speed_upward": jnp.clip(jax.random.uniform(part_keys[3], (MESH_POINTS_NORTH, MESH_POINTS_EAST, MESH_POINTS_UP, TRACER_TOTAL), jnp.float32, -0.3, 0.3) * block_scale(part_keys[3], (MESH_POINTS_NORTH, MESH_POINTS_EAST, MESH_POINTS_UP, TRACER_TOTAL), ((0, 2), (1, 2), (2, 2)), -0.4, 0.0), -0.3, 0.3),
    }


def strip_edges(values, dims):
    for dim in dims:
        values = lax.slice_in_dim(values, 1, values.shape[dim] - 1, axis=dim)
    return values


def neighbour(values, dim, start, dims):
    others = [other for other in dims if other != dim]
    values = strip_edges(values, others)
    return lax.slice_in_dim(values, start, start + values.shape[dim] - 2, axis=dim)


def march_once(padded_with_frame, scaled_speed_north, scaled_speed_east, scaled_speed_upward):
    middle = strip_edges(padded_with_frame, (0, 1, 2))
    lower = [neighbour(padded_with_frame, dim, 0, (0, 1, 2)) for dim in (0, 1, 2)]
    upper = [neighbour(padded_with_frame, dim, 2, (0, 1, 2)) for dim in (0, 1, 2)]
    slopes = [above - below for above, below in zip(upper, lower)]
    smooth_rate = 0.05
    spread = lower[0] + upper[0] + lower[1] + upper[1] + lower[2] + upper[2] - 6.0 * middle
    return middle - scaled_speed_north * slopes[0] - scaled_speed_east * slopes[1] - scaled_speed_upward * slopes[2] + smooth_rate * spread


def reference(initial_heat_state, scaled_speed_north, scaled_speed_east, scaled_speed_upward):
    for step in range(STEPS):
        initial_heat_state = march_once(jnp.pad(initial_heat_state, ((1, 1), (1, 1), (1, 1), (0, 0)), mode="constant"), scaled_speed_north, scaled_speed_east, scaled_speed_upward)
    return initial_heat_state
```

```python
import functools

import jax
import jax.numpy as jnp
from jax import lax
from jax.experimental import pallas as pl
from jax.experimental.pallas import tpu as pltpu
from jax.sharding import PartitionSpec as P

STEPS = 4
CUTS = ((0, 32, 64), (0, 32, 64), (0, 32, 64), (0, 32, 56, 62, 64))
PAD = 8
MESH = pl.DeviceIdType.MESH
AXES = ("py", "px", "pz")


def pieces(rows, t):
    ends = sorted({rows * cut // 64 for cut in CUTS[t]})
    return [(a, b - a) for a, b in zip(ends, ends[1:])]


def most(rows, parity):
    return max(len(pieces(rows, t)) for t in range(parity, STEPS, 2))


def kernel(
    counts, x, vn, ve, vu, out, s, w,
    edge_sem, load_sem, speed_sem,
    py_send, py_recv_even, py_recv_odd, px_send, px_recv, pz_send, pz_recv,
):
    planes, rows, depth, _ = x.shape
    parts = [pieces(rows, t) for t in range(STEPS)]
    cells = pl.ds(PAD, depth)
    speeds = (vn, ve, vu)
    py_recv = (py_recv_even, py_recv_odd)
    outer = sorted({1, planes})
    inner_count = planes - 2
    index = {axis: lax.axis_index(axis) for axis in AXES}

    def sends(axis, way):
        return index[axis] < counts[axis] - 1 if way == 0 else index[axis] > 0

    def receives(axis, way):
        return sends(axis, 1 - way)

    def target(axis, way):
        count = counts[axis]
        return {axis: lax.rem(index[axis] + (1 if way == 0 else count - 1), count)}

    def lane(axis, way):
        return way if counts[axis] > 2 else 0

    def remote(src, dst, send, recv, axis, way):
        return pltpu.make_async_remote_copy(
            src_ref=src, dst_ref=dst, send_sem=send, recv_sem=recv,
            device_id=target(axis, way), device_id_type=MESH,
        )

    def py_copy(way, t, i):
        first, span = parts[t][i]
        here = pl.ds(1 + first, span)
        src = s.at[t, planes if way == 0 else 1, here, cells]
        dst = s.at[t, 0 if way == 0 else planes + 1, here, cells]
        return remote(src, dst, py_send.at[lane("py", way)], py_recv[t % 2].at[lane("py", way), i], "py", way)

    def px_copy(way, t):
        row = rows if way == 0 else 1
        inner = pl.ds(1, planes)
        src = x.at[:, row - 1] if t == 0 else s.at[t, inner, row, cells]
        dst = s.at[t, inner, 0 if way == 0 else rows + 1, cells]
        return remote(src, dst, px_send.at[lane("px", way)], px_recv.at[lane("px", way), t % 2], "px", way)

    def pz_copy(way, t):
        inner, here = pl.ds(1, planes), pl.ds(1, rows)
        first = depth - PAD if way == 0 else 0
        if t == 0:
            src = x.at[:, :, pl.ds(first, PAD)]
        else:
            src = s.at[t, inner, here, pl.ds(PAD + first, PAD)]
        dst = s.at[t, inner, here, pl.ds(0 if way == 0 else PAD + depth, PAD)]
        return remote(src, dst, pz_send.at[lane("pz", way)], pz_recv.at[lane("pz", way), t % 2], "pz", way)

    def wait_sent():
        steps, inner, here = pl.ds(0, STEPS), pl.ds(1, planes), pl.ds(1, rows)

        def wait(axis, sem, block, way):
            pltpu.make_async_copy(block, block, sem.at[lane(axis, way)]).wait()

        each("py", sends, functools.partial(wait, "py", py_send, s.at[steps, 1, here, cells]))
        each("px", sends, functools.partial(wait, "px", px_send, s.at[steps, inner, 1, cells]))
        each("pz", sends, functools.partial(wait, "pz", pz_send, s.at[steps, inner, here, pl.ds(PAD, PAD)]))

    def each(axis, test, action):
        if counts[axis] > 1:
            for way in (0, 1):
                pl.when(test(axis, way))(functools.partial(action, way))

    def send_py(t, i):
        each("py", sends, lambda way: py_copy(way, t, i).start())

    def send_rest(t):
        each("px", sends, lambda way: px_copy(way, t).start())
        each("pz", sends, lambda way: pz_copy(way, t).start())

    def wait_py(t, i):
        each("py", receives, lambda way: py_copy(way, t, i).wait_recv())

    def wait_rest(t):
        each("px", receives, lambda way: px_copy(way, t).wait_recv())
        each("pz", receives, lambda way: pz_copy(way, t).wait_recv())

    def speed_copy(k, i):
        here = pl.ds(*parts[0][i])
        return pltpu.make_async_copy(speeds[k].at[:, here], w.at[k, :, here], speed_sem.at[i])

    def wait_speeds(i):
        block = w.at[:, :, pl.ds(*parts[0][i])]
        pltpu.make_async_copy(block, block, speed_sem.at[i]).wait()

    def edge_load(k, i):
        first, span = parts[0][i]
        return pltpu.make_async_copy(
            x.at[outer[k] - 1, pl.ds(first, span)],
            s.at[0, outer[k], pl.ds(1 + first, span), cells],
            edge_sem.at[k, i],
        )

    barrier = pltpu.get_barrier_semaphore()
    greeted = 0
    for axis in AXES:
        each(axis, sends, lambda way, axis=axis: pl.semaphore_signal(
            barrier, inc=1, device_id=target(axis, way), device_id_type=MESH))
        if counts[axis] > 1:
            for way in (0, 1):
                greeted = greeted + sends(axis, way).astype(jnp.int32)
    for i in range(len(parts[0])):
        for k in range(len(outer)):
            edge_load(k, i).start()
    if inner_count > 0:
        load = pltpu.make_async_copy(
            x.at[pl.ds(1, inner_count)],
            s.at[0, pl.ds(2, inner_count), pl.ds(1, rows), cells],
            load_sem,
        )
        load.start()

    pl.semaphore_wait(barrier, greeted)

    for i in range(len(parts[0])):
        for k in range(len(outer)):
            edge_load(k, i).wait()
        send_py(0, i)
    send_rest(0)
    for i in range(len(parts[0])):
        for k in range(3):
            speed_copy(k, i).start()

    def clear(axis, way):
        lanes = s.shape[-1]

        def fill(t, _):
            if axis == "py":
                plane = 0 if way == 0 else planes + 1

                def row_fill(r, _):
                    s[t, plane, 1 + r, PAD:PAD + depth, :] = jnp.zeros((depth, lanes), s.dtype)
                    return None

                lax.fori_loop(0, rows, row_fill, None)
            elif axis == "px":
                row = 0 if way == 0 else rows + 1
                for p in range(1, planes + 1):
                    s[t, p, row, PAD:PAD + depth, :] = jnp.zeros((depth, lanes), s.dtype)
            else:
                first = 0 if way == 0 else PAD + depth

                def row_fill(r, _):
                    for p in range(1, planes + 1):
                        s[t, p, 1 + r, first:first + PAD, :] = jnp.zeros((PAD, lanes), s.dtype)
                    return None

                lax.fori_loop(0, rows, row_fill, None)
            return None

        lax.fori_loop(0, STEPS, fill, None)

    for axis in AXES:
        for way in (0, 1):
            pl.when(jnp.logical_not(receives(axis, way)))(functools.partial(clear, axis, way))

    if inner_count > 0:
        load.wait()

    def update(t, piece, wanted):
        def row(r, _):
            for z in range(PAD, PAD + depth, 8):
                here = slice(z, z + 8)
                column = {}
                for p in wanted:
                    for q in (p, p + 1, p + 2):
                        if q not in column:
                            column[q] = s[t, q, r + 1, here, :]
                    lower = (column[p], s[t, p + 1, r, here, :], s[t, p + 1, r + 1, z - 1:z + 7, :])
                    upper = (column[p + 2], s[t, p + 1, r + 2, here, :], s[t, p + 1, r + 1, z + 1:z + 9, :])
                    middle = column[p + 1]
                    value = middle
                    for k in range(3):
                        value = value - w[k, p, r, z - PAD:z - PAD + 8, :] * (upper[k] - lower[k])
                    spread = (lower[0] + upper[0]) + (lower[1] + upper[1]) + (lower[2] + upper[2])
                    value = value + 0.05 * (spread - 6.0 * middle)
                    if t == STEPS - 1:
                        out[p, r, z - PAD:z - PAD + 8, :] = value
                    else:
                        s[t + 1, p + 1, r + 1, here, :] = value
            return None

        lax.fori_loop(piece[0], piece[0] + piece[1], row, None)

    for t in range(STEPS - 1):
        wait_rest(t)
        sent = 0
        for i, piece in enumerate(parts[t]):
            if t == 0:
                wait_speeds(i)
            wait_py(t, i)
            update(t, piece, range(planes))
            while sent < len(parts[t + 1]) and sum(parts[t + 1][sent]) <= sum(piece):
                send_py(t + 1, sent)
                sent += 1
        send_rest(t + 1)

    last = STEPS - 1
    wait_rest(last)
    update(last, (0, rows), range(1, planes - 1))
    split = planes > 1 and counts["py"] > 1
    if split:
        for way in (0, 1):
            pl.when(jnp.logical_not(receives("py", way)))(
                lambda way=way: update(last, (0, rows), [(planes - 1) * way]))
    for i, piece in enumerate(parts[last]):
        wait_py(last, i)
        if split:
            each("py", receives, lambda way: update(last, piece, [(planes - 1) * way]))
        else:
            update(last, piece, [p - 1 for p in outer])
    wait_sent()


def body(counts, x, vn, ve, vu):
    planes, rows, depth, lanes = x.shape
    first = len(pieces(rows, 0))
    ways = {axis: 2 if counts[axis] > 2 else 1 for axis in AXES}
    dma = pltpu.SemaphoreType.DMA
    return pl.pallas_call(
        functools.partial(kernel, counts),
        out_shape=pltpu.VMEM(x.shape, x.dtype),
        in_specs=[pl.BlockSpec(memory_space=pl.ANY)] * 4,
        out_specs=pl.BlockSpec(memory_space=pltpu.VMEM),
        scratch_shapes=[
            pltpu.VMEM((STEPS, planes + 2, rows + 2, depth + 2 * PAD, lanes), x.dtype),
            pltpu.VMEM((3, planes, rows, depth, lanes), x.dtype),
            dma((2, first)),
            dma(()),
            dma((first,)),
            dma((ways["py"],)),
            dma((ways["py"], most(rows, 0))),
            dma((ways["py"], most(rows, 1))),
            dma((ways["px"],)),
            dma((ways["px"], 2)),
            dma((ways["pz"],)),
            dma((ways["pz"], 2)),
        ],
        compiler_params=pltpu.CompilerParams(
            collective_id=0, has_side_effects=True, vmem_limit_bytes=54 * 2**20
        ),
    )(x, vn, ve, vu)


def solution(mesh):
    counts = {axis: mesh.shape[axis] for axis in ("py", "px", "pz")}
    spec = P(("site", "py"), "px", "pz", None)
    return jax.shard_map(
        functools.partial(body, counts), mesh=mesh, in_specs=(spec,) * 4, out_specs=spec,
        check_vma=False,
    )
```

```python
import functools

import jax
import jax.numpy as jnp
from jax import lax
from jax.experimental import pallas as pl
from jax.experimental.pallas import tpu as pltpu
from jax.sharding import PartitionSpec as P

STEPS = 4
CUTS = ((0, 32, 64), (0, 32, 64), (0, 32, 64), (0, 32, 56, 62, 64))
LOADS = (0, 4, 32, 64)
PAD = 8
MESH = pl.DeviceIdType.MESH
AXES = ("py", "px", "pz")


def pieces(rows, cuts):
    ends = sorted({rows * cut // 64 for cut in cuts})
    return [(a, b - a) for a, b in zip(ends, ends[1:])]


def most(rows, parity):
    return max(len(pieces(rows, CUTS[t])) for t in range(parity, STEPS, 2))


def kernel(
    counts, x, vn, ve, vu, out, s, w,
    hello, edge_sem, load_sem, speed_sem,
    py_send, py_recv_even, py_recv_odd, px_send, px_recv, pz_send, pz_recv,
):
    planes, rows, depth, _ = x.shape
    parts = [pieces(rows, CUTS[t]) for t in range(STEPS)]
    loads = pieces(rows, LOADS)
    cells = pl.ds(PAD, depth)
    speeds = (vn, ve, vu)
    py_recv = (py_recv_even, py_recv_odd)
    outer = sorted({1, planes})
    index = {axis: lax.axis_index(axis) for axis in AXES}

    def sends(axis, way):
        return index[axis] < counts[axis] - 1 if way == 0 else index[axis] > 0

    def receives(axis, way):
        return sends(axis, 1 - way)

    def target(axis, way):
        count = counts[axis]
        return {axis: lax.rem(index[axis] + (1 if way == 0 else count - 1), count)}

    def lane(axis, way):
        return way if counts[axis] > 2 else 0

    def remote(src, dst, send, recv, axis, way):
        return pltpu.make_async_remote_copy(
            src_ref=src, dst_ref=dst, send_sem=send, recv_sem=recv,
            device_id=target(axis, way), device_id_type=MESH,
        )

    def py_copy(way, t, i, piece=None):
        first, span = piece or parts[t][i]
        here = pl.ds(1 + first, span)
        src = s.at[t, planes if way == 0 else 1, here, cells]
        dst = s.at[t, 0 if way == 0 else planes + 1, here, cells]
        return remote(src, dst, py_send.at[lane("py", way)], py_recv[t % 2].at[lane("py", way), i], "py", way)

    def px_copy(way, t):
        row = rows if way == 0 else 1
        inner = pl.ds(1, planes)
        src = x.at[:, row - 1] if t == 0 else s.at[t, inner, row, cells]
        dst = s.at[t, inner, 0 if way == 0 else rows + 1, cells]
        return remote(src, dst, px_send.at[lane("px", way)], px_recv.at[lane("px", way), t % 2], "px", way)

    def pz_copy(way, t):
        inner, here = pl.ds(1, planes), pl.ds(1, rows)
        first = depth - PAD if way == 0 else 0
        if t == 0:
            src = x.at[:, :, pl.ds(first, PAD)]
        else:
            src = s.at[t, inner, here, pl.ds(PAD + first, PAD)]
        dst = s.at[t, inner, here, pl.ds(0 if way == 0 else PAD + depth, PAD)]
        return remote(src, dst, pz_send.at[lane("pz", way)], pz_recv.at[lane("pz", way), t % 2], "pz", way)

    def wait_sent():
        steps, inner, here = pl.ds(0, STEPS), pl.ds(1, planes), pl.ds(1, rows)

        def wait(axis, sem, block, way):
            pltpu.make_async_copy(block, block, sem.at[lane(axis, way)]).wait()

        each("py", sends, functools.partial(wait, "py", py_send, s.at[steps, 1, here, cells]))
        each("px", sends, functools.partial(wait, "px", px_send, s.at[steps, inner, 1, cells]))
        each("pz", sends, functools.partial(wait, "pz", pz_send, s.at[steps, inner, here, pl.ds(PAD, PAD)]))

    def each(axis, test, action):
        if counts[axis] > 1:
            for way in (0, 1):
                pl.when(test(axis, way))(functools.partial(action, way))

    def send_py(t, i):
        each("py", sends, lambda way: py_copy(way, t, i).start())

    def send_loaded(way, piece):
        i = max(i for i, part in enumerate(parts[0]) if part[0] <= piece[0])
        py_copy(way, 0, i, piece).start()

    def send_rest(t):
        each("px", sends, lambda way: px_copy(way, t).start())
        each("pz", sends, lambda way: pz_copy(way, t).start())

    def wait_py(t, i):
        each("py", receives, lambda way: py_copy(way, t, i).wait_recv())

    def wait_rest(t):
        each("px", receives, lambda way: px_copy(way, t).wait_recv())
        each("pz", receives, lambda way: pz_copy(way, t).wait_recv())

    def speed_copy(k, i):
        here = pl.ds(*parts[0][i])
        return pltpu.make_async_copy(speeds[k].at[:, here], w.at[k, :, here], speed_sem.at[i])

    def wait_speeds(i):
        block = w.at[:, :, pl.ds(*parts[0][i])]
        pltpu.make_async_copy(block, block, speed_sem.at[i]).wait()

    edge = jnp.where(sends("py", 0), planes, 1) if counts["py"] > 1 else planes

    def edge_load(i):
        first, span = loads[i]
        return pltpu.make_async_copy(
            x.at[edge - 1, pl.ds(first, span)],
            s.at[0, edge, pl.ds(1 + first, span), cells],
            edge_sem.at[i],
        )

    def rest_load():
        first = jnp.where(edge == 1, 1, 0)
        return pltpu.make_async_copy(
            x.at[pl.ds(first, planes - 1)],
            s.at[0, pl.ds(1 + first, planes - 1), pl.ds(1, rows), cells],
            load_sem,
        )

    def greet(axis, semaphore):
        each(axis, sends, lambda way: pl.semaphore_signal(
            semaphore, inc=1, device_id=target(axis, way), device_id_type=MESH))

    def peers(axis):
        if counts[axis] == 1:
            return 0
        return sum(sends(axis, way).astype(jnp.int32) for way in (0, 1))

    def odd(axis):
        return lax.rem(index[axis], 2) == 1

    def even(axis):
        return lax.rem(index[axis], 2) == 0

    side = [axis for axis in ("px", "pz") if counts[axis] > 1]
    barrier = pltpu.get_barrier_semaphore()
    greet("py", barrier)
    greeted = peers("py")
    for axis in side:
        pl.when(even(axis))(functools.partial(greet, axis, barrier))
        greeted = greeted + lax.rem(index[axis], 2) * peers(axis)
    for i in range(len(loads)):
        edge_load(i).start()
    if planes > 1:
        rest_load().start()

    both = jnp.logical_and(sends("py", 0), sends("py", 1)) if counts["py"] > 2 else jnp.bool_(False)

    pl.semaphore_wait(barrier, greeted)

    for i, piece in enumerate(loads):
        edge_load(i).wait()
        if counts["py"] > 1:
            pl.when(sends("py", 0))(lambda piece=piece: send_loaded(0, piece))
            pl.when(jnp.logical_not(sends("py", 0)))(lambda piece=piece: send_loaded(1, piece))
    if counts["py"] > 2:
        @pl.when(both)
        def _():
            if planes > 1:
                rest_load().wait()
            for piece in loads:
                send_loaded(1, piece)

    for k, axis in enumerate(side):
        pl.when(odd(axis))(functools.partial(greet, axis, hello.at[k]))
    for i in range(len(parts[0])):
        for k in range(3):
            speed_copy(k, i).start()
    for k, axis in enumerate(side):
        pl.when(even(axis))(lambda k=k, axis=axis: pl.semaphore_wait(hello.at[k], peers(axis)))
    send_rest(0)

    def clear(axis, way):
        lanes = s.shape[-1]

        def fill(t, _):
            if axis == "py":
                plane = 0 if way == 0 else planes + 1

                def row_fill(r, _):
                    s[t, plane, 1 + r, PAD:PAD + depth, :] = jnp.zeros((depth, lanes), s.dtype)
                    return None

                lax.fori_loop(0, rows, row_fill, None)
            elif axis == "px":
                row = 0 if way == 0 else rows + 1
                for p in range(1, planes + 1):
                    s[t, p, row, PAD:PAD + depth, :] = jnp.zeros((depth, lanes), s.dtype)
            else:
                first = 0 if way == 0 else PAD + depth

                def row_fill(r, _):
                    for p in range(1, planes + 1):
                        s[t, p, 1 + r, first:first + PAD, :] = jnp.zeros((PAD, lanes), s.dtype)
                    return None

                lax.fori_loop(0, rows, row_fill, None)
            return None

        lax.fori_loop(0, STEPS, fill, None)

    for axis in AXES:
        for way in (0, 1):
            pl.when(jnp.logical_not(receives(axis, way)))(functools.partial(clear, axis, way))

    if planes > 1:
        pl.when(jnp.logical_not(both))(lambda: rest_load().wait())

    def update(t, piece, wanted):
        def row(r, _):
            for z in range(PAD, PAD + depth, 8):
                here = slice(z, z + 8)
                column = {}
                for p in wanted:
                    for q in (p, p + 1, p + 2):
                        if q not in column:
                            column[q] = s[t, q, r + 1, here, :]
                    lower = (column[p], s[t, p + 1, r, here, :], s[t, p + 1, r + 1, z - 1:z + 7, :])
                    upper = (column[p + 2], s[t, p + 1, r + 2, here, :], s[t, p + 1, r + 1, z + 1:z + 9, :])
                    middle = column[p + 1]
                    value = middle
                    for k in range(3):
                        value = value - w[k, p, r, z - PAD:z - PAD + 8, :] * (upper[k] - lower[k])
                    spread = (lower[0] + upper[0]) + (lower[1] + upper[1]) + (lower[2] + upper[2])
                    value = value + 0.05 * (spread - 6.0 * middle)
                    if t == STEPS - 1:
                        out[p, r, z - PAD:z - PAD + 8, :] = value
                    else:
                        s[t + 1, p + 1, r + 1, here, :] = value
            return None

        lax.fori_loop(piece[0], piece[0] + piece[1], row, None)

    for t in range(STEPS - 1):
        wait_rest(t)
        sent = 0
        for i, piece in enumerate(parts[t]):
            if t == 0:
                wait_speeds(i)
            wait_py(t, i)
            update(t, piece, range(planes))
            while sent < len(parts[t + 1]) and sum(parts[t + 1][sent]) <= sum(piece):
                send_py(t + 1, sent)
                sent += 1
        send_rest(t + 1)

    last = STEPS - 1
    wait_rest(last)
    update(last, (0, rows), range(1, planes - 1))
    split = planes > 1 and counts["py"] > 1
    if split:
        for way in (0, 1):
            pl.when(jnp.logical_not(receives("py", way)))(
                lambda way=way: update(last, (0, rows), [(planes - 1) * way]))
    for i, piece in enumerate(parts[last]):
        wait_py(last, i)
        if split:
            each("py", receives, lambda way: update(last, piece, [(planes - 1) * way]))
        else:
            update(last, piece, [p - 1 for p in outer])
    wait_sent()


def body(counts, x, vn, ve, vu):
    planes, rows, depth, lanes = x.shape
    first = len(pieces(rows, CUTS[0]))
    ways = {axis: 2 if counts[axis] > 2 else 1 for axis in AXES}
    dma = pltpu.SemaphoreType.DMA
    return pl.pallas_call(
        functools.partial(kernel, counts),
        out_shape=pltpu.VMEM(x.shape, x.dtype),
        in_specs=[pl.BlockSpec(memory_space=pl.ANY)] * 4,
        out_specs=pl.BlockSpec(memory_space=pltpu.VMEM),
        scratch_shapes=[
            pltpu.VMEM((STEPS, planes + 2, rows + 2, depth + 2 * PAD, lanes), x.dtype),
            pltpu.VMEM((3, planes, rows, depth, lanes), x.dtype),
            pltpu.SemaphoreType.REGULAR((2,)),
            dma((len(pieces(rows, LOADS)),)),
            dma(()),
            dma((first,)),
            dma((ways["py"],)),
            dma((ways["py"], most(rows, 0))),
            dma((ways["py"], most(rows, 1))),
            dma((ways["px"],)),
            dma((ways["px"], 2)),
            dma((ways["pz"],)),
            dma((ways["pz"], 2)),
        ],
        compiler_params=pltpu.CompilerParams(
            collective_id=0, has_side_effects=True, vmem_limit_bytes=54 * 2**20
        ),
    )(x, vn, ve, vu)


def solution(mesh):
    counts = {axis: mesh.shape[axis] for axis in ("py", "px", "pz")}
    spec = P(("site", "py"), "px", "pz", None)
    return jax.shard_map(
        functools.partial(body, counts), mesh=mesh, in_specs=(spec,) * 4, out_specs=spec,
        check_vma=False,
    )
```

```python
import functools

import jax
import jax.numpy as jnp
from jax import lax
from jax.experimental import pallas as pl
from jax.experimental.pallas import tpu as pltpu
from jax.sharding import PartitionSpec as P

STEPS = 4
CUTS = ((0, 32, 64), (0, 32, 64), (0, 32, 64), (0, 32, 56, 62, 64))
LOADS = (0, 4, 32, 60, 64)
PAD = 8
MESH = pl.DeviceIdType.MESH
AXES = ("py", "px", "pz")


def pieces(rows, cuts):
    ends = sorted({rows * cut // 64 for cut in cuts})
    return [(a, b - a) for a, b in zip(ends, ends[1:])]


def most(rows, parity):
    return max(len(pieces(rows, CUTS[t])) for t in range(parity, STEPS, 2))


def kernel(
    counts, x, vn, ve, vu, out, s, w, via,
    hello, edge_sem, load_sem, speed_sem,
    py_send, py_recv_even, py_recv_odd, px_send, px_recv, pz_send, pz_recv,
    pass_send, pass_recv,
):
    planes, rows, depth, _ = x.shape
    parts = [pieces(rows, CUTS[t]) for t in range(STEPS)]
    loads = pieces(rows, LOADS)
    cells = pl.ds(PAD, depth)
    speeds = (vn, ve, vu)
    py_recv = (py_recv_even, py_recv_odd)
    outer = sorted({1, planes})
    index = {axis: lax.axis_index(axis) for axis in AXES}

    def sends(axis, way):
        return index[axis] < counts[axis] - 1 if way == 0 else index[axis] > 0

    def receives(axis, way):
        return sends(axis, 1 - way)

    def target(axis, way):
        count = counts[axis]
        return {axis: lax.rem(index[axis] + (1 if way == 0 else count - 1), count)}

    def lane(axis, way):
        return way if counts[axis] > 2 else 0

    def remote(src, dst, send, recv, axis, way):
        return pltpu.make_async_remote_copy(
            src_ref=src, dst_ref=dst, send_sem=send, recv_sem=recv,
            device_id=target(axis, way), device_id_type=MESH,
        )

    def py_copy(way, t, i, piece=None):
        first, span = piece or parts[t][i]
        here = pl.ds(1 + first, span)
        src = s.at[t, planes if way == 0 else 1, here, cells]
        dst = s.at[t, 0 if way == 0 else planes + 1, here, cells]
        return remote(src, dst, py_send.at[lane("py", way), min(t, 1)], py_recv[t % 2].at[lane("py", way), i], "py", way)

    def px_copy(way, t):
        row = rows if way == 0 else 1
        inner = pl.ds(1, planes)
        src = x.at[:, row - 1] if t == 0 else s.at[t, inner, row, cells]
        dst = s.at[t, inner, 0 if way == 0 else rows + 1, cells]
        return remote(src, dst, px_send.at[lane("px", way)], px_recv.at[lane("px", way), t % 2], "px", way)

    def pz_copy(way, t):
        inner, here = pl.ds(1, planes), pl.ds(1, rows)
        first = depth - PAD if way == 0 else 0
        if t == 0:
            src = x.at[:, :, pl.ds(first, PAD)]
        else:
            src = s.at[t, inner, here, pl.ds(PAD + first, PAD)]
        dst = s.at[t, inner, here, pl.ds(0 if way == 0 else PAD + depth, PAD)]
        return remote(src, dst, pz_send.at[lane("pz", way)], pz_recv.at[lane("pz", way), t % 2], "pz", way)

    def wait_sent():
        inner, here = pl.ds(1, planes), pl.ds(1, rows)
        every, later = pl.ds(0, STEPS), pl.ds(1, STEPS - 1)

        def wait(semaphore, block):
            pltpu.make_async_copy(block, block, semaphore).wait()

        def py_wait(way):
            def first_wait(span):
                wait(py_send.at[lane("py", way), 0], s.at[0, 1, pl.ds(1, span), cells])

            by_relay(way, lambda: first_wait(chunk[0]), lambda: first_wait(rows))
            wait(py_send.at[lane("py", way), 1], s.at[later, 1, here, cells])

        each("py", sends, py_wait)
        each("px", sends, lambda way: wait(px_send.at[lane("px", way)], s.at[every, inner, 1, cells]))
        each("pz", sends, lambda way: wait(
            pz_send.at[lane("pz", way)], s.at[every, inner, here, pl.ds(PAD, PAD)]))
        if relayed:
            pl.when(jnp.logical_or(hands, relays))(lambda: hop_in().wait_send())

    def each(axis, test, action):
        if counts[axis] > 1:
            for way in (0, 1):
                pl.when(test(axis, way))(functools.partial(action, way))

    def odd(axis):
        return lax.rem(index[axis], 2) == 1

    def even(axis):
        return lax.rem(index[axis], 2) == 0

    chunk = loads[-1]
    relayed = counts["py"] > 1 and counts["px"] > 1
    if relayed:
        front = index["pz"] == 0
        paired = jnp.logical_and(front, jnp.logical_and(even("px"), sends("px", 0)))
        hands = jnp.logical_and(paired, sends("py", 1))
        relays = jnp.logical_and(jnp.logical_and(front, odd("px")), sends("py", 1))

    def by_relay(way, yes, no):
        if relayed and way == 1:
            pl.when(paired)(yes)
            pl.when(jnp.logical_not(paired))(no)
        else:
            no()

    def hop(src, dst, device):
        return pltpu.make_async_remote_copy(
            src_ref=src, dst_ref=dst, send_sem=pass_send, recv_sem=pass_recv,
            device_id=device, device_id_type=MESH,
        )

    def hop_in():
        return hop(s.at[0, 1, pl.ds(1 + chunk[0], chunk[1]), cells], via, target("px", 0))

    def hop_out():
        landing = s.at[0, planes + 1, pl.ds(1 + chunk[0], chunk[1]), cells]
        return hop(via, landing, {**target("py", 1), **target("px", 1)})

    def send_py(t, i):
        each("py", sends, lambda way: py_copy(way, t, i).start())

    def send_loaded(way, piece):
        i = max(i for i, part in enumerate(parts[0]) if part[0] <= piece[0])
        start = lambda: py_copy(way, 0, i, piece).start()
        if piece == chunk:
            by_relay(way, lambda: None, start)
        else:
            start()

    def send_rest(t):
        each("px", sends, lambda way: px_copy(way, t).start())
        each("pz", sends, lambda way: pz_copy(way, t).start())

    def wait_py(t, i):
        def wait(way):
            whole = lambda: py_copy(way, t, i).wait_recv()

            def split():
                first = parts[0][i][0]
                py_copy(way, 0, i, (first, chunk[0] - first)).wait_recv()
                hop_out().wait_recv()

            if t == 0 and sum(parts[0][i]) == rows:
                by_relay(way, split, whole)
            else:
                whole()

        each("py", receives, wait)

    def wait_rest(t):
        each("px", receives, lambda way: px_copy(way, t).wait_recv())
        each("pz", receives, lambda way: pz_copy(way, t).wait_recv())

    def speed_copy(k, i):
        here = pl.ds(*parts[0][i])
        return pltpu.make_async_copy(speeds[k].at[:, here], w.at[k, :, here], speed_sem.at[i])

    def wait_speeds(i):
        block = w.at[:, :, pl.ds(*parts[0][i])]
        pltpu.make_async_copy(block, block, speed_sem.at[i]).wait()

    edge = jnp.where(sends("py", 0), planes, 1) if counts["py"] > 1 else planes

    def edge_load(i):
        first, span = loads[i]
        return pltpu.make_async_copy(
            x.at[edge - 1, pl.ds(first, span)],
            s.at[0, edge, pl.ds(1 + first, span), cells],
            edge_sem.at[i],
        )

    def rest_load():
        first = jnp.where(edge == 1, 1, 0)
        return pltpu.make_async_copy(
            x.at[pl.ds(first, planes - 1)],
            s.at[0, pl.ds(1 + first, planes - 1), pl.ds(1, rows), cells],
            load_sem,
        )

    def greet(axis, semaphore):
        each(axis, sends, lambda way: pl.semaphore_signal(
            semaphore, inc=1, device_id=target(axis, way), device_id_type=MESH))

    def peers(axis):
        if counts[axis] == 1:
            return 0
        return sum(sends(axis, way).astype(jnp.int32) for way in (0, 1))

    side = [axis for axis in ("px", "pz") if counts[axis] > 1]
    barrier = pltpu.get_barrier_semaphore()
    greet("py", barrier)
    greeted = peers("py")
    for axis in side:
        pl.when(even(axis))(functools.partial(greet, axis, barrier))
        greeted = greeted + lax.rem(index[axis], 2) * peers(axis)
    for i in range(len(loads)):
        edge_load(i).start()
    if planes > 1:
        rest_load().start()

    both = jnp.logical_and(sends("py", 0), sends("py", 1)) if counts["py"] > 2 else jnp.bool_(False)

    pl.semaphore_wait(barrier, greeted)

    for i, piece in enumerate(loads):
        edge_load(i).wait()
        if counts["py"] > 1:
            pl.when(sends("py", 0))(lambda piece=piece: send_loaded(0, piece))
            pl.when(jnp.logical_not(sends("py", 0)))(lambda piece=piece: send_loaded(1, piece))
    if counts["py"] > 2:
        @pl.when(both)
        def _():
            if planes > 1:
                rest_load().wait()
            for piece in loads:
                send_loaded(1, piece)

    for k, axis in enumerate(side):
        pl.when(odd(axis))(functools.partial(greet, axis, hello.at[k]))
    for i in range(len(parts[0])):
        for k in range(3):
            speed_copy(k, i).start()
    for k, axis in enumerate(side):
        pl.when(even(axis))(lambda k=k, axis=axis: pl.semaphore_wait(hello.at[k], peers(axis)))
    if relayed:
        pl.when(hands)(lambda: hop_in().start())
    send_rest(0)

    def clear(axis, way):
        lanes = s.shape[-1]

        def fill(t, _):
            if axis == "py":
                plane = 0 if way == 0 else planes + 1

                def row_fill(r, _):
                    s[t, plane, 1 + r, PAD:PAD + depth, :] = jnp.zeros((depth, lanes), s.dtype)
                    return None

                lax.fori_loop(0, rows, row_fill, None)
            elif axis == "px":
                row = 0 if way == 0 else rows + 1
                for p in range(1, planes + 1):
                    s[t, p, row, PAD:PAD + depth, :] = jnp.zeros((depth, lanes), s.dtype)
            else:
                first = 0 if way == 0 else PAD + depth

                def row_fill(r, _):
                    for p in range(1, planes + 1):
                        s[t, p, 1 + r, first:first + PAD, :] = jnp.zeros((PAD, lanes), s.dtype)
                    return None

                lax.fori_loop(0, rows, row_fill, None)
            return None

        lax.fori_loop(0, STEPS, fill, None)

    for axis in AXES:
        for way in (0, 1):
            pl.when(jnp.logical_not(receives(axis, way)))(functools.partial(clear, axis, way))

    if planes > 1:
        pl.when(jnp.logical_not(both))(lambda: rest_load().wait())

    if relayed:
        @pl.when(relays)
        def _():
            hop_in().wait_recv()
            hop_out().start()

    def update(t, piece, wanted):
        def row(r, _):
            for z in range(PAD, PAD + depth, 8):
                here = slice(z, z + 8)
                column = {}
                for p in wanted:
                    for q in (p, p + 1, p + 2):
                        if q not in column:
                            column[q] = s[t, q, r + 1, here, :]
                    lower = (column[p], s[t, p + 1, r, here, :], s[t, p + 1, r + 1, z - 1:z + 7, :])
                    upper = (column[p + 2], s[t, p + 1, r + 2, here, :], s[t, p + 1, r + 1, z + 1:z + 9, :])
                    middle = column[p + 1]
                    value = middle
                    for k in range(3):
                        value = value - w[k, p, r, z - PAD:z - PAD + 8, :] * (upper[k] - lower[k])
                    spread = (lower[0] + upper[0]) + (lower[1] + upper[1]) + (lower[2] + upper[2])
                    value = value + 0.05 * (spread - 6.0 * middle)
                    if t == STEPS - 1:
                        out[p, r, z - PAD:z - PAD + 8, :] = value
                    else:
                        s[t + 1, p + 1, r + 1, here, :] = value
            return None

        lax.fori_loop(piece[0], piece[0] + piece[1], row, None)

    for t in range(STEPS - 1):
        wait_rest(t)
        sent = 0
        for i, piece in enumerate(parts[t]):
            if t == 0:
                wait_speeds(i)
            wait_py(t, i)
            update(t, piece, range(planes))
            while sent < len(parts[t + 1]) and sum(parts[t + 1][sent]) <= sum(piece):
                send_py(t + 1, sent)
                sent += 1
        send_rest(t + 1)

    last = STEPS - 1
    wait_rest(last)
    update(last, (0, rows), range(1, planes - 1))
    split = planes > 1 and counts["py"] > 1
    if split:
        for way in (0, 1):
            pl.when(jnp.logical_not(receives("py", way)))(
                lambda way=way: update(last, (0, rows), [(planes - 1) * way]))
    for i, piece in enumerate(parts[last]):
        wait_py(last, i)
        if split:
            each("py", receives, lambda way: update(last, piece, [(planes - 1) * way]))
        else:
            update(last, piece, [p - 1 for p in outer])
    wait_sent()


def body(counts, x, vn, ve, vu):
    planes, rows, depth, lanes = x.shape
    first = len(pieces(rows, CUTS[0]))
    ways = {axis: 2 if counts[axis] > 2 else 1 for axis in AXES}
    dma = pltpu.SemaphoreType.DMA
    return pl.pallas_call(
        functools.partial(kernel, counts),
        out_shape=pltpu.VMEM(x.shape, x.dtype),
        in_specs=[pl.BlockSpec(memory_space=pl.ANY)] * 4,
        out_specs=pl.BlockSpec(memory_space=pltpu.VMEM),
        scratch_shapes=[
            pltpu.VMEM((STEPS, planes + 2, rows + 2, depth + 2 * PAD, lanes), x.dtype),
            pltpu.VMEM((3, planes, rows, depth, lanes), x.dtype),
            pltpu.VMEM((pieces(rows, LOADS)[-1][1], depth, lanes), x.dtype),
            pltpu.SemaphoreType.REGULAR((2,)),
            dma((len(pieces(rows, LOADS)),)),
            dma(()),
            dma((first,)),
            dma((ways["py"], 2)),
            dma((ways["py"], most(rows, 0))),
            dma((ways["py"], most(rows, 1))),
            dma((ways["px"],)),
            dma((ways["px"], 2)),
            dma((ways["pz"],)),
            dma((ways["pz"], 2)),
            dma(()),
            dma(()),
        ],
        compiler_params=pltpu.CompilerParams(
            collective_id=0, has_side_effects=True, vmem_limit_bytes=54 * 2**20
        ),
    )(x, vn, ve, vu)


def solution(mesh):
    counts = {axis: mesh.shape[axis] for axis in ("py", "px", "pz")}
    spec = P(("site", "py"), "px", "pz", None)
    return jax.shard_map(
        functools.partial(body, counts), mesh=mesh, in_specs=(spec,) * 4, out_specs=spec,
        check_vma=False,
    )
```

```python
import functools

import jax
import jax.numpy as jnp
from jax import lax
from jax.experimental import pallas as pl
from jax.experimental.pallas import tpu as pltpu
from jax.sharding import PartitionSpec as P

STEPS = 4
CUTS = ((0, 32, 64), (0, 32, 64), (0, 32, 64), (0, 32, 56, 62, 64))
LOADS = (0, 4, 32, 58, 64)
ROUTES = 3
PAD = 8
MESH = pl.DeviceIdType.MESH
AXES = ("py", "px", "pz")


def pieces(rows, cuts):
    ends = sorted({rows * cut // 64 for cut in cuts})
    return [(a, b - a) for a, b in zip(ends, ends[1:])]


def most(rows, parity):
    return max(len(pieces(rows, CUTS[t])) for t in range(parity, STEPS, 2))


def detours(counts):
    return min(ROUTES, counts["site"] - 1) if counts["py"] > 1 else 0


def kernel(
    counts, x, vn, ve, vu, out, s, w, via,
    hello, edge_sem, load_sem, speed_sem,
    py_send, py_recv_even, py_recv_odd, px_send, px_recv, pz_send, pz_recv,
    pass_send, pass_recv,
):
    planes, rows, depth, _ = x.shape
    parts = [pieces(rows, CUTS[t]) for t in range(STEPS)]
    loads = pieces(rows, LOADS)
    cells = pl.ds(PAD, depth)
    speeds = (vn, ve, vu)
    py_recv = (py_recv_even, py_recv_odd)
    outer = sorted({1, planes})
    index = {axis: lax.axis_index(axis) for axis in (*AXES, "site")}

    def sends(axis, way):
        return index[axis] < counts[axis] - 1 if way == 0 else index[axis] > 0

    def receives(axis, way):
        return sends(axis, 1 - way)

    def target(axis, way):
        count = counts[axis]
        return {axis: lax.rem(index[axis] + (1 if way == 0 else count - 1), count)}

    def lane(axis, way):
        return way if counts[axis] > 2 else 0

    def remote(src, dst, send, recv, axis, way):
        return pltpu.make_async_remote_copy(
            src_ref=src, dst_ref=dst, send_sem=send, recv_sem=recv,
            device_id=target(axis, way), device_id_type=MESH,
        )

    def py_copy(way, t, i, piece=None):
        first, span = piece or parts[t][i]
        here = pl.ds(1 + first, span)
        src = s.at[t, planes if way == 0 else 1, here, cells]
        dst = s.at[t, 0 if way == 0 else planes + 1, here, cells]
        return remote(src, dst, py_send.at[lane("py", way), min(t, 1)], py_recv[t % 2].at[lane("py", way), i], "py", way)

    def px_copy(way, t):
        row = rows if way == 0 else 1
        inner = pl.ds(1, planes)
        src = x.at[:, row - 1] if t == 0 else s.at[t, inner, row, cells]
        dst = s.at[t, inner, 0 if way == 0 else rows + 1, cells]
        return remote(src, dst, px_send.at[lane("px", way)], px_recv.at[lane("px", way), t % 2], "px", way)

    def pz_copy(way, t):
        inner, here = pl.ds(1, planes), pl.ds(1, rows)
        first = depth - PAD if way == 0 else 0
        if t == 0:
            src = x.at[:, :, pl.ds(first, PAD)]
        else:
            src = s.at[t, inner, here, pl.ds(PAD + first, PAD)]
        dst = s.at[t, inner, here, pl.ds(0 if way == 0 else PAD + depth, PAD)]
        return remote(src, dst, pz_send.at[lane("pz", way)], pz_recv.at[lane("pz", way), t % 2], "pz", way)

    def wait_sent():
        inner, here = pl.ds(1, planes), pl.ds(1, rows)
        every, later = pl.ds(0, STEPS), pl.ds(1, STEPS - 1)

        def wait(semaphore, block):
            pltpu.make_async_copy(block, block, semaphore).wait()

        def py_wait(way):
            def first_wait(span):
                wait(py_send.at[lane("py", way), 0], s.at[0, 1, pl.ds(1, span), cells])

            by_route(way, lambda: first_wait(rows), lambda: first_wait(chunk[0]))
            wait(py_send.at[lane("py", way), 1], s.at[later, 1, here, cells])

        each("py", sends, py_wait)
        each("px", sends, lambda way: wait(px_send.at[lane("px", way)], s.at[every, inner, 1, cells]))
        each("pz", sends, lambda way: wait(
            pz_send.at[lane("pz", way)], s.at[every, inner, here, pl.ds(PAD, PAD)]))
        if routes:
            pl.when(hands)(lambda: wait(pass_send, s.at[0, 1, pl.ds(1, chunk[1]), cells]))
        for k in range(routes):
            pl.when(relays[k])(lambda k=k: hop_out(k).wait_send())

    def each(axis, test, action):
        if counts[axis] > 1:
            for way in (0, 1):
                pl.when(test(axis, way))(functools.partial(action, way))

    def odd(axis):
        return lax.rem(index[axis], 2) == 1

    def even(axis):
        return lax.rem(index[axis], 2) == 0

    chunk, routes = loads[-1], detours(counts)
    front = jnp.logical_and(index["pz"] == 0, even("px"))
    late = jnp.logical_and(front, index["site"] == 0)
    hands = jnp.logical_and(late, sends("py", 1))
    takes = jnp.logical_and(late, receives("py", 1))
    twin = jnp.logical_and(front, receives("py", 1))
    relays = [jnp.logical_and(twin, index["site"] == k + 1) for k in range(routes)]

    def part(k):
        ends = [chunk[0] + chunk[1] * j // routes for j in (k, k + 1)]
        return ends[0], ends[1] - ends[0]

    def hop(k, src, dst, device):
        return pltpu.make_async_remote_copy(
            src_ref=src, dst_ref=dst, send_sem=pass_send, recv_sem=pass_recv.at[k],
            device_id=device, device_id_type=MESH,
        )

    def hop_in(k):
        first, span = part(k)
        src = s.at[0, 1, pl.ds(1 + first, span), cells]
        return hop(k, src, via.at[pl.ds(0, span)], {**target("py", 1), "site": k + 1})

    def hop_out(k):
        first, span = part(k)
        dst = s.at[0, planes + 1, pl.ds(1 + first, span), cells]
        return hop(k, via.at[pl.ds(0, span)], dst, {"site": 0})

    def by_route(way, straight, split):
        if way == 1 and routes:
            pl.when(late)(split)
            pl.when(jnp.logical_not(late))(straight)
        else:
            straight()

    def send_py(t, i):
        each("py", sends, lambda way: py_copy(way, t, i).start())

    def send_loaded(way, piece):
        i = max(i for i, part in enumerate(parts[0]) if part[0] <= piece[0])
        start = lambda: py_copy(way, 0, i, piece).start()
        if piece == chunk:
            by_route(way, start, lambda: None)
        else:
            start()

    def send_rest(t):
        each("px", sends, lambda way: px_copy(way, t).start())
        each("pz", sends, lambda way: pz_copy(way, t).start())

    def wait_py(t, i):
        def wait(way):
            def whole():
                py_copy(way, t, i).wait_recv()

            def split():
                first = parts[0][i][0]
                py_copy(way, 0, i, (first, chunk[0] - first)).wait_recv()
                for k in range(routes):
                    hop_out(k).wait_recv()

            if t == 0 and sum(parts[0][i]) == rows:
                by_route(way, whole, split)
            else:
                whole()

        each("py", receives, wait)

    def wait_rest(t):
        each("px", receives, lambda way: px_copy(way, t).wait_recv())
        each("pz", receives, lambda way: pz_copy(way, t).wait_recv())

    def speed_copy(k, i):
        here = pl.ds(*parts[0][i])
        return pltpu.make_async_copy(speeds[k].at[:, here], w.at[k, :, here], speed_sem.at[i])

    def wait_speeds(i):
        block = w.at[:, :, pl.ds(*parts[0][i])]
        pltpu.make_async_copy(block, block, speed_sem.at[i]).wait()

    edge = jnp.where(sends("py", 0), planes, 1) if counts["py"] > 1 else planes

    def edge_load(i):
        first, span = loads[i]
        return pltpu.make_async_copy(
            x.at[edge - 1, pl.ds(first, span)],
            s.at[0, edge, pl.ds(1 + first, span), cells],
            edge_sem.at[i],
        )

    def rest_load():
        first = jnp.where(edge == 1, 1, 0)
        return pltpu.make_async_copy(
            x.at[pl.ds(first, planes - 1)],
            s.at[0, pl.ds(1 + first, planes - 1), pl.ds(1, rows), cells],
            load_sem,
        )

    def greet(axis, semaphore):
        each(axis, sends, lambda way: pl.semaphore_signal(
            semaphore, inc=1, device_id=target(axis, way), device_id_type=MESH))

    def peers(axis):
        if counts[axis] == 1:
            return 0
        return sum(sends(axis, way).astype(jnp.int32) for way in (0, 1))

    side = [axis for axis in ("px", "pz") if counts[axis] > 1]
    barrier = pltpu.get_barrier_semaphore()
    greet("py", barrier)
    greeted = peers("py")
    for axis in side:
        pl.when(even(axis))(functools.partial(greet, axis, barrier))
        greeted = greeted + lax.rem(index[axis], 2) * peers(axis)
    for k in range(routes):
        pl.when(takes)(lambda k=k: pl.semaphore_signal(
            barrier, inc=1, device_id={"site": k + 1}, device_id_type=MESH))
        greeted = greeted + relays[k].astype(jnp.int32)
    for i in range(len(loads)):
        edge_load(i).start()
    if planes > 1:
        rest_load().start()

    both = jnp.logical_and(sends("py", 0), sends("py", 1)) if counts["py"] > 2 else jnp.bool_(False)

    pl.semaphore_wait(barrier, greeted)

    for i, piece in enumerate(loads):
        edge_load(i).wait()
        if counts["py"] > 1:
            pl.when(sends("py", 0))(lambda piece=piece: send_loaded(0, piece))
            pl.when(jnp.logical_not(sends("py", 0)))(lambda piece=piece: send_loaded(1, piece))
    if counts["py"] > 2:
        @pl.when(both)
        def _():
            if planes > 1:
                rest_load().wait()
            for piece in loads:
                send_loaded(1, piece)

    for k, axis in enumerate(side):
        pl.when(odd(axis))(functools.partial(greet, axis, hello.at[k]))
    for k in range(routes):
        pl.when(relays[k])(lambda: pl.semaphore_signal(
            hello.at[2], inc=1, device_id={"site": 0}, device_id_type=MESH))
    for i in range(len(parts[0])):
        for k in range(3):
            speed_copy(k, i).start()
    for k, axis in enumerate(side):
        pl.when(even(axis))(lambda k=k, axis=axis: pl.semaphore_wait(hello.at[k], peers(axis)))
    if routes:
        @pl.when(takes)
        def _():
            pl.semaphore_wait(hello.at[2], routes)
            pl.semaphore_signal(
                hello.at[3], inc=1, device_id=target("py", 0), device_id_type=MESH)

        @pl.when(hands)
        def _():
            pl.semaphore_wait(hello.at[3], 1)
            for k in range(routes):
                hop_in(k).start()

    send_rest(0)

    def clear(axis, way):
        lanes = s.shape[-1]

        def fill(t, _):
            if axis == "py":
                plane = 0 if way == 0 else planes + 1

                def row_fill(r, _):
                    s[t, plane, 1 + r, PAD:PAD + depth, :] = jnp.zeros((depth, lanes), s.dtype)
                    return None

                lax.fori_loop(0, rows, row_fill, None)
            elif axis == "px":
                row = 0 if way == 0 else rows + 1
                for p in range(1, planes + 1):
                    s[t, p, row, PAD:PAD + depth, :] = jnp.zeros((depth, lanes), s.dtype)
            else:
                first = 0 if way == 0 else PAD + depth

                def row_fill(r, _):
                    for p in range(1, planes + 1):
                        s[t, p, 1 + r, first:first + PAD, :] = jnp.zeros((PAD, lanes), s.dtype)
                    return None

                lax.fori_loop(0, rows, row_fill, None)
            return None

        lax.fori_loop(0, STEPS, fill, None)

    for axis in AXES:
        for way in (0, 1):
            pl.when(jnp.logical_not(receives(axis, way)))(functools.partial(clear, axis, way))

    if planes > 1:
        pl.when(jnp.logical_not(both))(lambda: rest_load().wait())

    for k in range(routes):
        @pl.when(relays[k])
        def _(k=k):
            hop_in(k).wait_recv()
            hop_out(k).start()

    def update(t, piece, wanted):
        def row(r, _):
            for z in range(PAD, PAD + depth, 8):
                here = slice(z, z + 8)
                column = {}
                for p in wanted:
                    for q in (p, p + 1, p + 2):
                        if q not in column:
                            column[q] = s[t, q, r + 1, here, :]
                    lower = (column[p], s[t, p + 1, r, here, :], s[t, p + 1, r + 1, z - 1:z + 7, :])
                    upper = (column[p + 2], s[t, p + 1, r + 2, here, :], s[t, p + 1, r + 1, z + 1:z + 9, :])
                    middle = column[p + 1]
                    value = middle
                    for k in range(3):
                        value = value - w[k, p, r, z - PAD:z - PAD + 8, :] * (upper[k] - lower[k])
                    spread = (lower[0] + upper[0]) + (lower[1] + upper[1]) + (lower[2] + upper[2])
                    value = value + 0.05 * (spread - 6.0 * middle)
                    if t == STEPS - 1:
                        out[p, r, z - PAD:z - PAD + 8, :] = value
                    else:
                        s[t + 1, p + 1, r + 1, here, :] = value
            return None

        lax.fori_loop(piece[0], piece[0] + piece[1], row, None)

    for t in range(STEPS - 1):
        wait_rest(t)
        sent = 0
        for i, piece in enumerate(parts[t]):
            if t == 0:
                wait_speeds(i)
            wait_py(t, i)
            update(t, piece, range(planes))
            while sent < len(parts[t + 1]) and sum(parts[t + 1][sent]) <= sum(piece):
                send_py(t + 1, sent)
                sent += 1
        send_rest(t + 1)

    last = STEPS - 1
    wait_rest(last)
    update(last, (0, rows), range(1, planes - 1))
    split = planes > 1 and counts["py"] > 1
    if split:
        for way in (0, 1):
            pl.when(jnp.logical_not(receives("py", way)))(
                lambda way=way: update(last, (0, rows), [(planes - 1) * way]))
    for i, piece in enumerate(parts[last]):
        wait_py(last, i)
        if split:
            each("py", receives, lambda way: update(last, piece, [(planes - 1) * way]))
        else:
            update(last, piece, [p - 1 for p in outer])
    wait_sent()


def body(counts, x, vn, ve, vu):
    planes, rows, depth, lanes = x.shape
    first = len(pieces(rows, CUTS[0]))
    ways = {axis: 2 if counts[axis] > 2 else 1 for axis in AXES}
    dma = pltpu.SemaphoreType.DMA
    return pl.pallas_call(
        functools.partial(kernel, counts),
        out_shape=pltpu.VMEM(x.shape, x.dtype),
        in_specs=[pl.BlockSpec(memory_space=pl.ANY)] * 4,
        out_specs=pl.BlockSpec(memory_space=pltpu.VMEM),
        scratch_shapes=[
            pltpu.VMEM((STEPS, planes + 2, rows + 2, depth + 2 * PAD, lanes), x.dtype),
            pltpu.VMEM((3, planes, rows, depth, lanes), x.dtype),
            pltpu.VMEM((pieces(rows, LOADS)[-1][1], depth, lanes), x.dtype),
            pltpu.SemaphoreType.REGULAR((4,)),
            dma((len(pieces(rows, LOADS)),)),
            dma(()),
            dma((first,)),
            dma((ways["py"], 2)),
            dma((ways["py"], most(rows, 0))),
            dma((ways["py"], most(rows, 1))),
            dma((ways["px"],)),
            dma((ways["px"], 2)),
            dma((ways["pz"],)),
            dma((ways["pz"], 2)),
            dma(()),
            dma((max(detours(counts), 1),)),
        ],
        compiler_params=pltpu.CompilerParams(
            collective_id=0, has_side_effects=True, vmem_limit_bytes=54 * 2**20
        ),
    )(x, vn, ve, vu)


def solution(mesh):
    counts = {axis: mesh.shape[axis] for axis in (*AXES, "site")}
    spec = P(("site", "py"), "px", "pz", None)
    return jax.shard_map(
        functools.partial(body, counts), mesh=mesh, in_specs=(spec,) * 4, out_specs=spec,
        check_vma=False,
    )
```

```python
import functools

import jax
import jax.numpy as jnp
from jax import lax
from jax.experimental import pallas as pl
from jax.experimental.pallas import tpu as pltpu
from jax.sharding import PartitionSpec as P

STEPS = 4
CUTS = ((0, 32, 64), (0, 32, 64), (0, 32, 64), (0, 32, 56, 62, 64))
LOADS = (0, 4, 32, 58, 64)
ROUTES = 3
PAD = 8
MESH = pl.DeviceIdType.MESH
AXES = ("py", "px", "pz")


def pieces(rows, cuts):
    ends = sorted({rows * cut // 64 for cut in cuts})
    return [(a, b - a) for a, b in zip(ends, ends[1:])]


def most(rows, parity):
    return max(len(pieces(rows, CUTS[t])) for t in range(parity, STEPS, 2))


def detours(counts):
    return min(ROUTES, counts["site"] - 1) if counts["py"] > 1 else 0


def kernel(
    counts, x, vn, ve, vu, out, s, w, via,
    hello, edge_sem, load_sem,
    py_send, py_recv_even, py_recv_odd, px_send, px_recv, pz_send, pz_recv,
    pass_send, pass_recv,
):
    planes, rows, depth, _ = x.shape
    parts = [pieces(rows, CUTS[t]) for t in range(STEPS)]
    loads = pieces(rows, LOADS)
    cells = pl.ds(PAD, depth)
    speeds = (vn, ve, vu)
    py_recv = (py_recv_even, py_recv_odd)
    outer = sorted({1, planes})
    index = {axis: lax.axis_index(axis) for axis in (*AXES, "site")}

    def sends(axis, way):
        return index[axis] < counts[axis] - 1 if way == 0 else index[axis] > 0

    def receives(axis, way):
        return sends(axis, 1 - way)

    def target(axis, way):
        count = counts[axis]
        return {axis: lax.rem(index[axis] + (1 if way == 0 else count - 1), count)}

    def lane(axis, way):
        return way if counts[axis] > 2 else 0

    def remote(src, dst, send, recv, axis, way):
        return pltpu.make_async_remote_copy(
            src_ref=src, dst_ref=dst, send_sem=send, recv_sem=recv,
            device_id=target(axis, way), device_id_type=MESH,
        )

    def py_copy(way, t, i, piece=None):
        first, span = piece or parts[t][i]
        here = pl.ds(1 + first, span)
        src = s.at[t, planes if way == 0 else 1, here, cells]
        dst = s.at[t, 0 if way == 0 else planes + 1, here, cells]
        return remote(src, dst, py_send.at[lane("py", way), min(t, 1)], py_recv[t % 2].at[lane("py", way), i], "py", way)

    def px_copy(way, t):
        row = rows if way == 0 else 1
        inner = pl.ds(1, planes)
        src = x.at[:, row - 1] if t == 0 else s.at[t, inner, row, cells]
        dst = s.at[t, inner, 0 if way == 0 else rows + 1, cells]
        return remote(src, dst, px_send.at[lane("px", way)], px_recv.at[lane("px", way), t % 2], "px", way)

    def pz_copy(way, t):
        inner, here = pl.ds(1, planes), pl.ds(1, rows)
        first = depth - PAD if way == 0 else 0
        if t == 0:
            src = x.at[:, :, pl.ds(first, PAD)]
        else:
            src = s.at[t, inner, here, pl.ds(PAD + first, PAD)]
        dst = s.at[t, inner, here, pl.ds(0 if way == 0 else PAD + depth, PAD)]
        return remote(src, dst, pz_send.at[lane("pz", way)], pz_recv.at[lane("pz", way), t % 2], "pz", way)

    def wait_sent():
        inner, here = pl.ds(1, planes), pl.ds(1, rows)
        every, later = pl.ds(0, STEPS), pl.ds(1, STEPS - 1)

        def wait(semaphore, block):
            pltpu.make_async_copy(block, block, semaphore).wait()

        def py_wait(way):
            def first_wait(span):
                wait(py_send.at[lane("py", way), 0], s.at[0, 1, pl.ds(1, span), cells])

            by_route(way, lambda: first_wait(rows), lambda: first_wait(chunk[0]))
            wait(py_send.at[lane("py", way), 1], s.at[later, 1, here, cells])

        each("py", sends, py_wait)
        each("px", sends, lambda way: wait(px_send.at[lane("px", way)], s.at[every, inner, 1, cells]))
        each("pz", sends, lambda way: wait(
            pz_send.at[lane("pz", way)], s.at[every, inner, here, pl.ds(PAD, PAD)]))
        if routes:
            pl.when(hands)(lambda: wait(pass_send, s.at[0, 1, pl.ds(1, chunk[1]), cells]))
        for k in range(routes):
            pl.when(relays[k])(lambda k=k: hop_out(k).wait_send())

    def each(axis, test, action):
        if counts[axis] > 1:
            for way in (0, 1):
                pl.when(test(axis, way))(functools.partial(action, way))

    def odd(axis):
        return lax.rem(index[axis], 2) == 1

    def even(axis):
        return lax.rem(index[axis], 2) == 0

    chunk, routes = loads[-1], detours(counts)
    front = jnp.logical_and(index["pz"] == 0, even("px"))
    late = jnp.logical_and(front, index["site"] == 0)
    hands = jnp.logical_and(late, sends("py", 1))
    takes = jnp.logical_and(late, receives("py", 1))
    twin = jnp.logical_and(front, receives("py", 1))
    relays = [jnp.logical_and(twin, index["site"] == k + 1) for k in range(routes)]

    def part(k):
        ends = [chunk[0] + chunk[1] * j // routes for j in (k, k + 1)]
        return ends[0], ends[1] - ends[0]

    def hop(src, dst, device):
        return pltpu.make_async_remote_copy(
            src_ref=src, dst_ref=dst, send_sem=pass_send, recv_sem=pass_recv,
            device_id=device, device_id_type=MESH,
        )

    def hop_in(k):
        first, span = part(k)
        src = s.at[0, 1, pl.ds(1 + first, span), cells]
        return hop(src, via.at[pl.ds(0, span)], {**target("py", 1), "site": k + 1})

    def hop_out(k):
        first, span = part(k)
        dst = s.at[0, planes + 1, pl.ds(1 + first, span), cells]
        return hop(via.at[pl.ds(0, span)], dst, {"site": 0})

    def by_route(way, straight, split):
        if way == 1 and routes:
            pl.when(late)(split)
            pl.when(jnp.logical_not(late))(straight)
        else:
            straight()

    def send_py(t, i):
        each("py", sends, lambda way: py_copy(way, t, i).start())

    def send_loaded(way, piece):
        i = max(i for i, part in enumerate(parts[0]) if part[0] <= piece[0])
        start = lambda: py_copy(way, 0, i, piece).start()
        if piece == chunk:
            by_route(way, start, lambda: None)
        else:
            start()

    def send_rest(t):
        each("px", sends, lambda way: px_copy(way, t).start())
        each("pz", sends, lambda way: pz_copy(way, t).start())

    def wait_py(t, i):
        def wait(way):
            def whole():
                py_copy(way, t, i).wait_recv()

            def split():
                first = parts[0][i][0]
                py_copy(way, 0, i, (first, chunk[0] - first)).wait_recv()
                block = s.at[0, planes + 1, pl.ds(1 + chunk[0], chunk[1]), cells]
                pltpu.make_async_copy(block, block, pass_recv).wait()

            if t == 0 and sum(parts[0][i]) == rows:
                by_route(way, whole, split)
            else:
                whole()

        each("py", receives, wait)

    def wait_rest(t):
        each("px", receives, lambda way: px_copy(way, t).wait_recv())
        each("pz", receives, lambda way: pz_copy(way, t).wait_recv())

    def speed_copy(k, i):
        here = pl.ds(*parts[0][i])
        return pltpu.make_async_copy(speeds[k].at[:, here], w.at[k, :, here], edge_sem.at[i])

    def wait_speeds(i):
        block = w.at[:, :, pl.ds(*parts[0][i])]
        pltpu.make_async_copy(block, block, edge_sem.at[i]).wait()

    edge = jnp.where(sends("py", 0), planes, 1) if counts["py"] > 1 else planes

    def edge_load(i):
        first, span = loads[i]
        return pltpu.make_async_copy(
            x.at[edge - 1, pl.ds(first, span)],
            s.at[0, edge, pl.ds(1 + first, span), cells],
            edge_sem.at[i],
        )

    def rest_load():
        first = jnp.where(edge == 1, 1, 0)
        return pltpu.make_async_copy(
            x.at[pl.ds(first, planes - 1)],
            s.at[0, pl.ds(1 + first, planes - 1), pl.ds(1, rows), cells],
            load_sem,
        )

    def greet(axis, semaphore):
        each(axis, sends, lambda way: pl.semaphore_signal(
            semaphore, inc=1, device_id=target(axis, way), device_id_type=MESH))

    def peers(axis):
        if counts[axis] == 1:
            return 0
        return sum(sends(axis, way).astype(jnp.int32) for way in (0, 1))

    for i in range(len(loads)):
        edge_load(i).start()
    if planes > 1:
        rest_load().start()

    side = [axis for axis in ("px", "pz") if counts[axis] > 1]
    barrier = pltpu.get_barrier_semaphore()
    greet("py", barrier)
    greeted = peers("py")
    for axis in side:
        pl.when(even(axis))(functools.partial(greet, axis, barrier))
        greeted = greeted + lax.rem(index[axis], 2) * peers(axis)
    for k in range(routes):
        pl.when(takes)(lambda k=k: pl.semaphore_signal(
            barrier, inc=1, device_id={"site": k + 1}, device_id_type=MESH))
        greeted = greeted + relays[k].astype(jnp.int32)
    both = jnp.logical_and(sends("py", 0), sends("py", 1)) if counts["py"] > 2 else jnp.bool_(False)

    pl.semaphore_wait(barrier, greeted)

    for i, piece in enumerate(loads):
        edge_load(i).wait()
        if counts["py"] > 1:
            pl.when(sends("py", 0))(lambda piece=piece: send_loaded(0, piece))
            pl.when(jnp.logical_not(sends("py", 0)))(lambda piece=piece: send_loaded(1, piece))
    if counts["py"] > 2:
        @pl.when(both)
        def _():
            if planes > 1:
                rest_load().wait()
            for piece in loads:
                send_loaded(1, piece)

    for axis in side:
        pl.when(odd(axis))(functools.partial(greet, axis, hello.at[0]))
    for k in range(routes):
        pl.when(relays[k])(lambda: pl.semaphore_signal(
            hello.at[0], inc=1, device_id={"site": 0}, device_id_type=MESH))
    for i in range(len(parts[0])):
        for k in range(3):
            speed_copy(k, i).start()
    answers = sum((1 - lax.rem(index[axis], 2)) * peers(axis) for axis in side)
    answers = answers + routes * takes.astype(jnp.int32)
    if side or routes:
        pl.when(answers > 0)(lambda: pl.semaphore_wait(hello.at[0], answers))
    if routes:
        @pl.when(takes)
        def _():
            pl.semaphore_signal(
                hello.at[1], inc=1, device_id=target("py", 0), device_id_type=MESH)

        @pl.when(hands)
        def _():
            pl.semaphore_wait(hello.at[1], 1)
            for k in range(routes):
                hop_in(k).start()

    send_rest(0)

    def clear(axis, way):
        lanes = s.shape[-1]

        def fill(t, _):
            if axis == "py":
                plane = 0 if way == 0 else planes + 1

                def row_fill(r, _):
                    s[t, plane, 1 + r, PAD:PAD + depth, :] = jnp.zeros((depth, lanes), s.dtype)
                    return None

                lax.fori_loop(0, rows, row_fill, None)
            elif axis == "px":
                row = 0 if way == 0 else rows + 1
                for p in range(1, planes + 1):
                    s[t, p, row, PAD:PAD + depth, :] = jnp.zeros((depth, lanes), s.dtype)
            else:
                first = 0 if way == 0 else PAD + depth

                def row_fill(r, _):
                    for p in range(1, planes + 1):
                        s[t, p, 1 + r, first:first + PAD, :] = jnp.zeros((PAD, lanes), s.dtype)
                    return None

                lax.fori_loop(0, rows, row_fill, None)
            return None

        lax.fori_loop(0, STEPS, fill, None)

    for axis in AXES:
        for way in (0, 1):
            pl.when(jnp.logical_not(receives(axis, way)))(functools.partial(clear, axis, way))

    if planes > 1:
        pl.when(jnp.logical_not(both))(lambda: rest_load().wait())

    for k in range(routes):
        @pl.when(relays[k])
        def _(k=k):
            hop_in(k).wait_recv()
            hop_out(k).start()

    def update(t, piece, wanted):
        def row(r, _):
            for z in range(PAD, PAD + depth, 8):
                here = slice(z, z + 8)
                column = {}
                for p in wanted:
                    for q in (p, p + 1, p + 2):
                        if q not in column:
                            column[q] = s[t, q, r + 1, here, :]
                    lower = (column[p], s[t, p + 1, r, here, :], s[t, p + 1, r + 1, z - 1:z + 7, :])
                    upper = (column[p + 2], s[t, p + 1, r + 2, here, :], s[t, p + 1, r + 1, z + 1:z + 9, :])
                    middle = column[p + 1]
                    value = middle
                    for k in range(3):
                        value = value - w[k, p, r, z - PAD:z - PAD + 8, :] * (upper[k] - lower[k])
                    spread = (lower[0] + upper[0]) + (lower[1] + upper[1]) + (lower[2] + upper[2])
                    value = value + 0.05 * (spread - 6.0 * middle)
                    if t == STEPS - 1:
                        out[p, r, z - PAD:z - PAD + 8, :] = value
                    else:
                        s[t + 1, p + 1, r + 1, here, :] = value
            return None

        lax.fori_loop(piece[0], piece[0] + piece[1], row, None)

    for t in range(STEPS - 1):
        wait_rest(t)
        sent = 0
        for i, piece in enumerate(parts[t]):
            if t == 0:
                wait_speeds(i)
            wait_py(t, i)
            update(t, piece, range(planes))
            while sent < len(parts[t + 1]) and sum(parts[t + 1][sent]) <= sum(piece):
                send_py(t + 1, sent)
                sent += 1
        send_rest(t + 1)

    last = STEPS - 1
    wait_rest(last)
    update(last, (0, rows), range(1, planes - 1))
    split = planes > 1 and counts["py"] > 1
    if split:
        for way in (0, 1):
            pl.when(jnp.logical_not(receives("py", way)))(
                lambda way=way: update(last, (0, rows), [(planes - 1) * way]))
    for i, piece in enumerate(parts[last]):
        wait_py(last, i)
        if split:
            each("py", receives, lambda way: update(last, piece, [(planes - 1) * way]))
        else:
            update(last, piece, [p - 1 for p in outer])
    wait_sent()


def body(counts, x, vn, ve, vu):
    planes, rows, depth, lanes = x.shape
    ways = {axis: 2 if counts[axis] > 2 else 1 for axis in AXES}
    dma = pltpu.SemaphoreType.DMA
    return pl.pallas_call(
        functools.partial(kernel, counts),
        out_shape=pltpu.VMEM(x.shape, x.dtype),
        in_specs=[pl.BlockSpec(memory_space=pl.ANY)] * 4,
        out_specs=pl.BlockSpec(memory_space=pltpu.VMEM),
        scratch_shapes=[
            pltpu.VMEM((STEPS, planes + 2, rows + 2, depth + 2 * PAD, lanes), x.dtype),
            pltpu.VMEM((3, planes, rows, depth, lanes), x.dtype),
            pltpu.VMEM((pieces(rows, LOADS)[-1][1], depth, lanes), x.dtype),
            pltpu.SemaphoreType.REGULAR((2,)),
            dma((max(len(pieces(rows, LOADS)), len(pieces(rows, CUTS[0]))),)),
            dma(()),
            dma((ways["py"], 2)),
            dma((ways["py"], most(rows, 0))),
            dma((ways["py"], most(rows, 1))),
            dma((ways["px"],)),
            dma((ways["px"], 2)),
            dma((ways["pz"],)),
            dma((ways["pz"], 2)),
            dma(()),
            dma(()),
        ],
        compiler_params=pltpu.CompilerParams(
            collective_id=0, has_side_effects=True, vmem_limit_bytes=54 * 2**20
        ),
    )(x, vn, ve, vu)


def solution(mesh):
    counts = {axis: mesh.shape[axis] for axis in (*AXES, "site")}
    spec = P(("site", "py"), "px", "pz", None)
    return jax.shard_map(
        functools.partial(body, counts), mesh=mesh, in_specs=(spec,) * 4, out_specs=spec,
        check_vma=False,
    )
```

```python
import functools

import jax
import jax.numpy as jnp
from jax import lax
from jax.experimental import pallas as pl
from jax.experimental.pallas import tpu as pltpu
from jax.sharding import PartitionSpec as P

STEPS = 4
CUTS = ((0, 32, 64), (0, 32, 64), (0, 32, 64), (0, 32, 52, 60, 63, 64))
LOADS = (0, 4, 32, 58, 64)
ROUTES = 3
PAD = 8
MESH = pl.DeviceIdType.MESH
AXES = ("py", "px", "pz")


def pieces(rows, cuts):
    ends = sorted({rows * cut // 64 for cut in cuts})
    return [(a, b - a) for a, b in zip(ends, ends[1:])]


def most(rows, parity):
    return max(len(pieces(rows, CUTS[t])) for t in range(parity, STEPS, 2))


def detours(counts):
    return min(ROUTES, counts["site"] - 1) if counts["py"] > 1 else 0


def kernel(
    counts, x, vn, ve, vu, out, s, w, via,
    hello, edge_sem, load_sem,
    py_send, py_recv_even, py_recv_odd, px_send, px_recv, pz_send, pz_recv,
    pass_send, pass_recv,
):
    planes, rows, depth, _ = x.shape
    parts = [pieces(rows, CUTS[t]) for t in range(STEPS)]
    loads = pieces(rows, LOADS)
    cells = pl.ds(PAD, depth)
    speeds = (vn, ve, vu)
    py_recv = (py_recv_even, py_recv_odd)
    outer = sorted({1, planes})
    index = {axis: lax.axis_index(axis) for axis in (*AXES, "site")}

    def sends(axis, way):
        return index[axis] < counts[axis] - 1 if way == 0 else index[axis] > 0

    def receives(axis, way):
        return sends(axis, 1 - way)

    def target(axis, way):
        count = counts[axis]
        return {axis: lax.rem(index[axis] + (1 if way == 0 else count - 1), count)}

    def lane(axis, way):
        return way if counts[axis] > 2 else 0

    def remote(src, dst, send, recv, axis, way):
        return pltpu.make_async_remote_copy(
            src_ref=src, dst_ref=dst, send_sem=send, recv_sem=recv,
            device_id=target(axis, way), device_id_type=MESH,
        )

    def py_copy(way, t, i, piece=None):
        first, span = piece or parts[t][i]
        here = pl.ds(1 + first, span)
        src = s.at[t, planes if way == 0 else 1, here, cells]
        dst = s.at[t, 0 if way == 0 else planes + 1, here, cells]
        return remote(src, dst, py_send.at[lane("py", way), min(t, 1)], py_recv[t % 2].at[lane("py", way), i], "py", way)

    def px_copy(way, t):
        row = rows if way == 0 else 1
        inner = pl.ds(1, planes)
        src = x.at[:, row - 1] if t == 0 else s.at[t, inner, row, cells]
        dst = s.at[t, inner, 0 if way == 0 else rows + 1, cells]
        return remote(src, dst, px_send.at[lane("px", way)], px_recv.at[lane("px", way), t % 2], "px", way)

    def pz_copy(way, t):
        inner, here = pl.ds(1, planes), pl.ds(1, rows)
        first = depth - PAD if way == 0 else 0
        if t == 0:
            src = x.at[:, :, pl.ds(first, PAD)]
        else:
            src = s.at[t, inner, here, pl.ds(PAD + first, PAD)]
        dst = s.at[t, inner, here, pl.ds(0 if way == 0 else PAD + depth, PAD)]
        return remote(src, dst, pz_send.at[lane("pz", way)], pz_recv.at[lane("pz", way), t % 2], "pz", way)

    def wait_sent():
        inner, here = pl.ds(1, planes), pl.ds(1, rows)
        every, later = pl.ds(0, STEPS), pl.ds(1, STEPS - 1)

        def wait(semaphore, block):
            pltpu.make_async_copy(block, block, semaphore).wait()

        def py_wait(way):
            def first_wait(span):
                wait(py_send.at[lane("py", way), 0], s.at[0, 1, pl.ds(1, span), cells])

            by_route(way, lambda: first_wait(rows), lambda: first_wait(chunk[0]))
            wait(py_send.at[lane("py", way), 1], s.at[later, 1, here, cells])

        each("py", sends, py_wait)
        each("px", sends, lambda way: wait(px_send.at[lane("px", way)], s.at[every, inner, 1, cells]))
        each("pz", sends, lambda way: wait(
            pz_send.at[lane("pz", way)], s.at[every, inner, here, pl.ds(PAD, PAD)]))
        if routes:
            pl.when(hands)(lambda: wait(pass_send, s.at[0, 1, pl.ds(1, chunk[1]), cells]))
        for k in range(routes):
            pl.when(relays[k])(lambda k=k: hop_out(k).wait_send())

    def each(axis, test, action):
        if counts[axis] > 1:
            for way in (0, 1):
                pl.when(test(axis, way))(functools.partial(action, way))

    def odd(axis):
        return lax.rem(index[axis], 2) == 1

    def even(axis):
        return lax.rem(index[axis], 2) == 0

    chunk, routes = loads[-1], detours(counts)
    front = jnp.logical_and(index["pz"] == 0, even("px"))
    late = jnp.logical_and(front, index["site"] == 0)
    hands = jnp.logical_and(late, sends("py", 1))
    takes = jnp.logical_and(late, receives("py", 1))
    twin = jnp.logical_and(front, receives("py", 1))
    relays = [jnp.logical_and(twin, index["site"] == k + 1) for k in range(routes)]

    def part(k):
        ends = [chunk[0] + chunk[1] * j // routes for j in (k, k + 1)]
        return ends[0], ends[1] - ends[0]

    def hop(src, dst, device):
        return pltpu.make_async_remote_copy(
            src_ref=src, dst_ref=dst, send_sem=pass_send, recv_sem=pass_recv,
            device_id=device, device_id_type=MESH,
        )

    def hop_in(k):
        first, span = part(k)
        src = s.at[0, 1, pl.ds(1 + first, span), cells]
        return hop(src, via.at[pl.ds(0, span)], {**target("py", 1), "site": k + 1})

    def hop_out(k):
        first, span = part(k)
        dst = s.at[0, planes + 1, pl.ds(1 + first, span), cells]
        return hop(via.at[pl.ds(0, span)], dst, {"site": 0})

    def by_route(way, straight, split):
        if way == 1 and routes:
            pl.when(late)(split)
            pl.when(jnp.logical_not(late))(straight)
        else:
            straight()

    def send_py(t, i):
        each("py", sends, lambda way: py_copy(way, t, i).start())

    def send_loaded(way, piece):
        i = max(i for i, part in enumerate(parts[0]) if part[0] <= piece[0])
        start = lambda: py_copy(way, 0, i, piece).start()
        if piece == chunk:
            by_route(way, start, lambda: None)
        else:
            start()

    def send_rest(t):
        each("px", sends, lambda way: px_copy(way, t).start())
        each("pz", sends, lambda way: pz_copy(way, t).start())

    def wait_py(t, i):
        def wait(way):
            def whole():
                py_copy(way, t, i).wait_recv()

            def split():
                first = parts[0][i][0]
                py_copy(way, 0, i, (first, chunk[0] - first)).wait_recv()
                block = s.at[0, planes + 1, pl.ds(1 + chunk[0], chunk[1]), cells]
                pltpu.make_async_copy(block, block, pass_recv).wait()

            if t == 0 and sum(parts[0][i]) == rows:
                by_route(way, whole, split)
            else:
                whole()

        each("py", receives, wait)

    def wait_rest(t):
        each("px", receives, lambda way: px_copy(way, t).wait_recv())
        each("pz", receives, lambda way: pz_copy(way, t).wait_recv())

    def speed_copy(k, i):
        here = pl.ds(*parts[0][i])
        return pltpu.make_async_copy(speeds[k].at[:, here], w.at[k, :, here], edge_sem.at[i])

    def wait_speeds(i):
        block = w.at[:, :, pl.ds(*parts[0][i])]
        pltpu.make_async_copy(block, block, edge_sem.at[i]).wait()

    edge = jnp.where(sends("py", 0), planes, 1) if counts["py"] > 1 else planes

    def edge_load(i):
        first, span = loads[i]
        return pltpu.make_async_copy(
            x.at[edge - 1, pl.ds(first, span)],
            s.at[0, edge, pl.ds(1 + first, span), cells],
            edge_sem.at[i],
        )

    def rest_load():
        first = jnp.where(edge == 1, 1, 0)
        return pltpu.make_async_copy(
            x.at[pl.ds(first, planes - 1)],
            s.at[0, pl.ds(1 + first, planes - 1), pl.ds(1, rows), cells],
            load_sem,
        )

    def greet(axis, semaphore):
        each(axis, sends, lambda way: pl.semaphore_signal(
            semaphore, inc=1, device_id=target(axis, way), device_id_type=MESH))

    def peers(axis):
        if counts[axis] == 1:
            return 0
        return sum(sends(axis, way).astype(jnp.int32) for way in (0, 1))

    for i in range(len(loads)):
        edge_load(i).start()
    if planes > 1:
        rest_load().start()

    side = [axis for axis in ("px", "pz") if counts[axis] > 1]
    barrier = pltpu.get_barrier_semaphore()
    greet("py", barrier)
    greeted = peers("py")
    for axis in side:
        pl.when(even(axis))(functools.partial(greet, axis, barrier))
        greeted = greeted + lax.rem(index[axis], 2) * peers(axis)
    for k in range(routes):
        pl.when(takes)(lambda k=k: pl.semaphore_signal(
            barrier, inc=1, device_id={"site": k + 1}, device_id_type=MESH))
        greeted = greeted + relays[k].astype(jnp.int32)
    both = jnp.logical_and(sends("py", 0), sends("py", 1)) if counts["py"] > 2 else jnp.bool_(False)

    pl.semaphore_wait(barrier, greeted)

    for i, piece in enumerate(loads):
        edge_load(i).wait()
        if counts["py"] > 1:
            pl.when(sends("py", 0))(lambda piece=piece: send_loaded(0, piece))
            pl.when(jnp.logical_not(sends("py", 0)))(lambda piece=piece: send_loaded(1, piece))
    if counts["py"] > 2:
        @pl.when(both)
        def _():
            if planes > 1:
                rest_load().wait()
            for piece in loads:
                send_loaded(1, piece)

    for axis in side:
        pl.when(odd(axis))(functools.partial(greet, axis, hello.at[0]))
    for k in range(routes):
        pl.when(relays[k])(lambda: pl.semaphore_signal(
            hello.at[0], inc=1, device_id={"site": 0}, device_id_type=MESH))
    for i in range(len(parts[0])):
        for k in range(3):
            speed_copy(k, i).start()
    answers = sum((1 - lax.rem(index[axis], 2)) * peers(axis) for axis in side)
    answers = answers + routes * takes.astype(jnp.int32)
    if side or routes:
        pl.when(answers > 0)(lambda: pl.semaphore_wait(hello.at[0], answers))
    if routes:
        @pl.when(takes)
        def _():
            pl.semaphore_signal(
                hello.at[1], inc=1, device_id=target("py", 0), device_id_type=MESH)

        @pl.when(hands)
        def _():
            pl.semaphore_wait(hello.at[1], 1)
            for k in range(routes):
                hop_in(k).start()

    send_rest(0)

    def clear(axis, way):
        lanes = s.shape[-1]

        def fill(t, _):
            if axis == "py":
                plane = 0 if way == 0 else planes + 1

                def row_fill(r, _):
                    s[t, plane, 1 + r, PAD:PAD + depth, :] = jnp.zeros((depth, lanes), s.dtype)
                    return None

                lax.fori_loop(0, rows, row_fill, None)
            elif axis == "px":
                row = 0 if way == 0 else rows + 1
                for p in range(1, planes + 1):
                    s[t, p, row, PAD:PAD + depth, :] = jnp.zeros((depth, lanes), s.dtype)
            else:
                first = 0 if way == 0 else PAD + depth

                def row_fill(r, _):
                    for p in range(1, planes + 1):
                        s[t, p, 1 + r, first:first + PAD, :] = jnp.zeros((PAD, lanes), s.dtype)
                    return None

                lax.fori_loop(0, rows, row_fill, None)
            return None

        lax.fori_loop(0, STEPS, fill, None)

    for axis in AXES:
        for way in (0, 1):
            pl.when(jnp.logical_not(receives(axis, way)))(functools.partial(clear, axis, way))

    if planes > 1:
        pl.when(jnp.logical_not(both))(lambda: rest_load().wait())

    for k in range(routes):
        @pl.when(relays[k])
        def _(k=k):
            hop_in(k).wait_recv()
            hop_out(k).start()

    def update(t, piece, wanted):
        def row(r, _):
            for z in range(PAD, PAD + depth, 8):
                here = slice(z, z + 8)
                column = {}
                for p in wanted:
                    for q in (p, p + 1, p + 2):
                        if q not in column:
                            column[q] = s[t, q, r + 1, here, :]
                    lower = (column[p], s[t, p + 1, r, here, :], s[t, p + 1, r + 1, z - 1:z + 7, :])
                    upper = (column[p + 2], s[t, p + 1, r + 2, here, :], s[t, p + 1, r + 1, z + 1:z + 9, :])
                    middle = column[p + 1]
                    value = middle
                    for k in range(3):
                        value = value - w[k, p, r, z - PAD:z - PAD + 8, :] * (upper[k] - lower[k])
                    spread = (lower[0] + upper[0]) + (lower[1] + upper[1]) + (lower[2] + upper[2])
                    value = value + 0.05 * (spread - 6.0 * middle)
                    if t == STEPS - 1:
                        out[p, r, z - PAD:z - PAD + 8, :] = value
                    else:
                        s[t + 1, p + 1, r + 1, here, :] = value
            return None

        lax.fori_loop(piece[0], piece[0] + piece[1], row, None)

    for t in range(STEPS - 1):
        wait_rest(t)
        sent = 0
        for i, piece in enumerate(parts[t]):
            if t == 0:
                wait_speeds(i)
            wait_py(t, i)
            update(t, piece, range(planes))
            while sent < len(parts[t + 1]) and sum(parts[t + 1][sent]) <= sum(piece):
                send_py(t + 1, sent)
                sent += 1
        send_rest(t + 1)

    last = STEPS - 1
    wait_rest(last)
    update(last, (0, rows), range(1, planes - 1))
    split = planes > 1 and counts["py"] > 1
    if split:
        for way in (0, 1):
            pl.when(jnp.logical_not(receives("py", way)))(
                lambda way=way: update(last, (0, rows), [(planes - 1) * way]))
    for i, piece in enumerate(parts[last]):
        wait_py(last, i)
        if split:
            each("py", receives, lambda way: update(last, piece, [(planes - 1) * way]))
        else:
            update(last, piece, [p - 1 for p in outer])
    wait_sent()


def body(counts, x, vn, ve, vu):
    planes, rows, depth, lanes = x.shape
    ways = {axis: 2 if counts[axis] > 2 else 1 for axis in AXES}
    dma = pltpu.SemaphoreType.DMA
    return pl.pallas_call(
        functools.partial(kernel, counts),
        out_shape=pltpu.VMEM(x.shape, x.dtype),
        in_specs=[pl.BlockSpec(memory_space=pl.ANY)] * 4,
        out_specs=pl.BlockSpec(memory_space=pltpu.VMEM),
        scratch_shapes=[
            pltpu.VMEM((STEPS, planes + 2, rows + 2, depth + 2 * PAD, lanes), x.dtype),
            pltpu.VMEM((3, planes, rows, depth, lanes), x.dtype),
            pltpu.VMEM((pieces(rows, LOADS)[-1][1], depth, lanes), x.dtype),
            pltpu.SemaphoreType.REGULAR((2,)),
            dma((max(len(pieces(rows, LOADS)), len(pieces(rows, CUTS[0]))),)),
            dma(()),
            dma((ways["py"], 2)),
            dma((ways["py"], most(rows, 0))),
            dma((ways["py"], most(rows, 1))),
            dma((ways["px"],)),
            dma((ways["px"], 2)),
            dma((ways["pz"],)),
            dma((ways["pz"], 2)),
            dma(()),
            dma(()),
        ],
        compiler_params=pltpu.CompilerParams(
            collective_id=0, has_side_effects=True, vmem_limit_bytes=54 * 2**20
        ),
    )(x, vn, ve, vu)


def solution(mesh):
    counts = {axis: mesh.shape[axis] for axis in (*AXES, "site")}
    spec = P(("site", "py"), "px", "pz", None)
    return jax.shard_map(
        functools.partial(body, counts), mesh=mesh, in_specs=(spec,) * 4, out_specs=spec,
        check_vma=False,
    )
```

```python
import functools

import jax
import jax.numpy as jnp
from jax import lax
from jax.experimental import pallas as pl
from jax.experimental.pallas import tpu as pltpu
from jax.sharding import PartitionSpec as P

STEPS = 4
CUTS = ((0, 32, 64), (0, 32, 64), (0, 32, 64), (0, 32, 52, 60, 63, 64))
LOADS = (0, 2, 32, 58, 64)
ROUTES = 3
PAD = 8
MESH = pl.DeviceIdType.MESH
AXES = ("py", "px", "pz")


def pieces(rows, cuts):
    ends = sorted({rows * cut // 64 for cut in cuts})
    return [(a, b - a) for a, b in zip(ends, ends[1:])]


def most(rows, parity):
    return max(len(pieces(rows, CUTS[t])) for t in range(parity, STEPS, 2))


def detours(counts):
    return min(ROUTES, counts["site"] - 1) if counts["py"] > 1 else 0


def kernel(
    counts, x, vn, ve, vu, out, s, w, via,
    hello, edge_sem, load_sem,
    py_send, py_recv_even, py_recv_odd, px_send, px_recv, pz_send, pz_recv,
    pass_send, pass_recv,
):
    planes, rows, depth, _ = x.shape
    parts = [pieces(rows, CUTS[t]) for t in range(STEPS)]
    loads = pieces(rows, LOADS)
    cells = pl.ds(PAD, depth)
    speeds = (vn, ve, vu)
    py_recv = (py_recv_even, py_recv_odd)
    outer = sorted({1, planes})
    index = {axis: lax.axis_index(axis) for axis in (*AXES, "site")}

    def sends(axis, way):
        return index[axis] < counts[axis] - 1 if way == 0 else index[axis] > 0

    def receives(axis, way):
        return sends(axis, 1 - way)

    def target(axis, way):
        count = counts[axis]
        return {axis: lax.rem(index[axis] + (1 if way == 0 else count - 1), count)}

    def lane(axis, way):
        return way if counts[axis] > 2 else 0

    def remote(src, dst, send, recv, axis, way):
        return pltpu.make_async_remote_copy(
            src_ref=src, dst_ref=dst, send_sem=send, recv_sem=recv,
            device_id=target(axis, way), device_id_type=MESH,
        )

    def py_copy(way, t, i, piece=None):
        first, span = piece or parts[t][i]
        here = pl.ds(1 + first, span)
        src = s.at[t, planes if way == 0 else 1, here, cells]
        dst = s.at[t, 0 if way == 0 else planes + 1, here, cells]
        return remote(src, dst, py_send.at[lane("py", way), min(t, 1)], py_recv[t % 2].at[lane("py", way), i], "py", way)

    def px_copy(way, t):
        row = rows if way == 0 else 1
        inner = pl.ds(1, planes)
        src = x.at[:, row - 1] if t == 0 else s.at[t, inner, row, cells]
        dst = s.at[t, inner, 0 if way == 0 else rows + 1, cells]
        return remote(src, dst, px_send.at[lane("px", way)], px_recv.at[lane("px", way), t % 2], "px", way)

    def pz_copy(way, t):
        inner, here = pl.ds(1, planes), pl.ds(1, rows)
        first = depth - PAD if way == 0 else 0
        if t == 0:
            src = x.at[:, :, pl.ds(first, PAD)]
        else:
            src = s.at[t, inner, here, pl.ds(PAD + first, PAD)]
        dst = s.at[t, inner, here, pl.ds(0 if way == 0 else PAD + depth, PAD)]
        return remote(src, dst, pz_send.at[lane("pz", way)], pz_recv.at[lane("pz", way), t % 2], "pz", way)

    def wait_sent():
        inner, here = pl.ds(1, planes), pl.ds(1, rows)
        every, later = pl.ds(0, STEPS), pl.ds(1, STEPS - 1)

        def wait(semaphore, block):
            pltpu.make_async_copy(block, block, semaphore).wait()

        def py_wait(way):
            def first_wait(span):
                wait(py_send.at[lane("py", way), 0], s.at[0, 1, pl.ds(1, span), cells])

            by_route(way, lambda: first_wait(rows), lambda: first_wait(chunk[0]))
            wait(py_send.at[lane("py", way), 1], s.at[later, 1, here, cells])

        each("py", sends, py_wait)
        each("px", sends, lambda way: wait(px_send.at[lane("px", way)], s.at[every, inner, 1, cells]))
        each("pz", sends, lambda way: wait(
            pz_send.at[lane("pz", way)], s.at[every, inner, here, pl.ds(PAD, PAD)]))
        if routes:
            pl.when(hands)(lambda: wait(pass_send, s.at[0, 1, pl.ds(1, chunk[1]), cells]))
        for k in range(routes):
            pl.when(relays[k])(lambda k=k: hop_out(k).wait_send())

    def each(axis, test, action):
        if counts[axis] > 1:
            for way in (0, 1):
                pl.when(test(axis, way))(functools.partial(action, way))

    def odd(axis):
        return lax.rem(index[axis], 2) == 1

    def even(axis):
        return lax.rem(index[axis], 2) == 0

    chunk, routes = loads[-1], detours(counts)
    front = jnp.logical_and(index["pz"] == 0, even("px"))
    late = jnp.logical_and(front, index["site"] == 0)
    hands = jnp.logical_and(late, sends("py", 1))
    takes = jnp.logical_and(late, receives("py", 1))
    twin = jnp.logical_and(front, receives("py", 1))
    relays = [jnp.logical_and(twin, index["site"] == k + 1) for k in range(routes)]

    def part(k):
        ends = [chunk[0] + chunk[1] * j // routes for j in (k, k + 1)]
        return ends[0], ends[1] - ends[0]

    def hop(src, dst, device):
        return pltpu.make_async_remote_copy(
            src_ref=src, dst_ref=dst, send_sem=pass_send, recv_sem=pass_recv,
            device_id=device, device_id_type=MESH,
        )

    def hop_in(k):
        first, span = part(k)
        src = s.at[0, 1, pl.ds(1 + first, span), cells]
        return hop(src, via.at[pl.ds(0, span)], {**target("py", 1), "site": k + 1})

    def hop_out(k):
        first, span = part(k)
        dst = s.at[0, planes + 1, pl.ds(1 + first, span), cells]
        return hop(via.at[pl.ds(0, span)], dst, {"site": 0})

    def by_route(way, straight, split):
        if way == 1 and routes:
            pl.when(late)(split)
            pl.when(jnp.logical_not(late))(straight)
        else:
            straight()

    def send_py(t, i):
        each("py", sends, lambda way: py_copy(way, t, i).start())

    def send_loaded(way, piece):
        i = max(i for i, part in enumerate(parts[0]) if part[0] <= piece[0])
        start = lambda: py_copy(way, 0, i, piece).start()
        if piece == chunk:
            by_route(way, start, lambda: None)
        else:
            start()

    def send_rest(t):
        each("px", sends, lambda way: px_copy(way, t).start())
        each("pz", sends, lambda way: pz_copy(way, t).start())

    def wait_py(t, i):
        def wait(way):
            def whole():
                py_copy(way, t, i).wait_recv()

            def split():
                first = parts[0][i][0]
                py_copy(way, 0, i, (first, chunk[0] - first)).wait_recv()
                block = s.at[0, planes + 1, pl.ds(1 + chunk[0], chunk[1]), cells]
                pltpu.make_async_copy(block, block, pass_recv).wait()

            if t == 0 and sum(parts[0][i]) == rows:
                by_route(way, whole, split)
            else:
                whole()

        each("py", receives, wait)

    def wait_rest(t):
        each("px", receives, lambda way: px_copy(way, t).wait_recv())
        each("pz", receives, lambda way: pz_copy(way, t).wait_recv())

    def speed_copy(k, i):
        here = pl.ds(*parts[0][i])
        return pltpu.make_async_copy(speeds[k].at[:, here], w.at[k, :, here], edge_sem.at[i])

    def wait_speeds(i):
        block = w.at[:, :, pl.ds(*parts[0][i])]
        pltpu.make_async_copy(block, block, edge_sem.at[i]).wait()

    edge = jnp.where(sends("py", 0), planes, 1) if counts["py"] > 1 else planes

    def edge_load(i):
        first, span = loads[i]
        return pltpu.make_async_copy(
            x.at[edge - 1, pl.ds(first, span)],
            s.at[0, edge, pl.ds(1 + first, span), cells],
            edge_sem.at[i],
        )

    def rest_load():
        first = jnp.where(edge == 1, 1, 0)
        return pltpu.make_async_copy(
            x.at[pl.ds(first, planes - 1)],
            s.at[0, pl.ds(1 + first, planes - 1), pl.ds(1, rows), cells],
            load_sem,
        )

    def greet(axis, semaphore):
        each(axis, sends, lambda way: pl.semaphore_signal(
            semaphore, inc=1, device_id=target(axis, way), device_id_type=MESH))

    def peers(axis):
        if counts[axis] == 1:
            return 0
        return sum(sends(axis, way).astype(jnp.int32) for way in (0, 1))

    for i in range(len(loads)):
        edge_load(i).start()
    if planes > 1:
        rest_load().start()

    side = [axis for axis in ("px", "pz") if counts[axis] > 1]
    barrier = pltpu.get_barrier_semaphore()
    greet("py", barrier)
    greeted = peers("py")
    for axis in side:
        pl.when(even(axis))(functools.partial(greet, axis, barrier))
        greeted = greeted + lax.rem(index[axis], 2) * peers(axis)
    for k in range(routes):
        pl.when(takes)(lambda k=k: pl.semaphore_signal(
            barrier, inc=1, device_id={"site": k + 1}, device_id_type=MESH))
        greeted = greeted + relays[k].astype(jnp.int32)
    both = jnp.logical_and(sends("py", 0), sends("py", 1)) if counts["py"] > 2 else jnp.bool_(False)

    pl.semaphore_wait(barrier, greeted)

    for i, piece in enumerate(loads):
        edge_load(i).wait()
        if counts["py"] > 1:
            pl.when(sends("py", 0))(lambda piece=piece: send_loaded(0, piece))
            pl.when(jnp.logical_not(sends("py", 0)))(lambda piece=piece: send_loaded(1, piece))
    if counts["py"] > 2:
        @pl.when(both)
        def _():
            if planes > 1:
                rest_load().wait()
            for piece in loads:
                send_loaded(1, piece)

    for axis in side:
        pl.when(odd(axis))(functools.partial(greet, axis, hello.at[0]))
    for k in range(routes):
        pl.when(relays[k])(lambda: pl.semaphore_signal(
            hello.at[0], inc=1, device_id={"site": 0}, device_id_type=MESH))
    for i in range(len(parts[0])):
        for k in range(3):
            speed_copy(k, i).start()
    answers = sum((1 - lax.rem(index[axis], 2)) * peers(axis) for axis in side)
    answers = answers + routes * takes.astype(jnp.int32)
    if side or routes:
        pl.when(answers > 0)(lambda: pl.semaphore_wait(hello.at[0], answers))
    if routes:
        @pl.when(takes)
        def _():
            pl.semaphore_signal(
                hello.at[1], inc=1, device_id=target("py", 0), device_id_type=MESH)

        @pl.when(hands)
        def _():
            pl.semaphore_wait(hello.at[1], 1)
            for k in range(routes):
                hop_in(k).start()

    send_rest(0)

    def clear(axis, way):
        lanes = s.shape[-1]

        def fill(t, _):
            if axis == "py":
                plane = 0 if way == 0 else planes + 1

                def row_fill(r, _):
                    s[t, plane, 1 + r, PAD:PAD + depth, :] = jnp.zeros((depth, lanes), s.dtype)
                    return None

                lax.fori_loop(0, rows, row_fill, None)
            elif axis == "px":
                row = 0 if way == 0 else rows + 1
                for p in range(1, planes + 1):
                    s[t, p, row, PAD:PAD + depth, :] = jnp.zeros((depth, lanes), s.dtype)
            else:
                first = 0 if way == 0 else PAD + depth

                def row_fill(r, _):
                    for p in range(1, planes + 1):
                        s[t, p, 1 + r, first:first + PAD, :] = jnp.zeros((PAD, lanes), s.dtype)
                    return None

                lax.fori_loop(0, rows, row_fill, None)
            return None

        lax.fori_loop(0, STEPS, fill, None)

    for axis in AXES:
        for way in (0, 1):
            pl.when(jnp.logical_not(receives(axis, way)))(functools.partial(clear, axis, way))

    if planes > 1:
        pl.when(jnp.logical_not(both))(lambda: rest_load().wait())

    for k in range(routes):
        @pl.when(relays[k])
        def _(k=k):
            hop_in(k).wait_recv()
            hop_out(k).start()

    def update(t, piece, wanted):
        def row(r, _):
            for z in range(PAD, PAD + depth, 8):
                here = slice(z, z + 8)
                column = {}
                for p in wanted:
                    for q in (p, p + 1, p + 2):
                        if q not in column:
                            column[q] = s[t, q, r + 1, here, :]
                    lower = (column[p], s[t, p + 1, r, here, :], s[t, p + 1, r + 1, z - 1:z + 7, :])
                    upper = (column[p + 2], s[t, p + 1, r + 2, here, :], s[t, p + 1, r + 1, z + 1:z + 9, :])
                    middle = column[p + 1]
                    value = middle
                    for k in range(3):
                        value = value - w[k, p, r, z - PAD:z - PAD + 8, :] * (upper[k] - lower[k])
                    spread = (lower[0] + upper[0]) + (lower[1] + upper[1]) + (lower[2] + upper[2])
                    value = value + 0.05 * (spread - 6.0 * middle)
                    if t == STEPS - 1:
                        out[p, r, z - PAD:z - PAD + 8, :] = value
                    else:
                        s[t + 1, p + 1, r + 1, here, :] = value
            return None

        lax.fori_loop(piece[0], piece[0] + piece[1], row, None)

    for t in range(STEPS - 1):
        wait_rest(t)
        sent = 0
        for i, piece in enumerate(parts[t]):
            if t == 0:
                wait_speeds(i)
            wait_py(t, i)
            update(t, piece, range(planes))
            while sent < len(parts[t + 1]) and sum(parts[t + 1][sent]) <= sum(piece):
                send_py(t + 1, sent)
                sent += 1
        send_rest(t + 1)

    last = STEPS - 1
    wait_rest(last)
    update(last, (0, rows), range(1, planes - 1))
    split = planes > 1 and counts["py"] > 1
    if split:
        for way in (0, 1):
            pl.when(jnp.logical_not(receives("py", way)))(
                lambda way=way: update(last, (0, rows), [(planes - 1) * way]))
    for i, piece in enumerate(parts[last]):
        wait_py(last, i)
        if split:
            each("py", receives, lambda way: update(last, piece, [(planes - 1) * way]))
        else:
            update(last, piece, [p - 1 for p in outer])
    wait_sent()


def body(counts, x, vn, ve, vu):
    planes, rows, depth, lanes = x.shape
    ways = {axis: 2 if counts[axis] > 2 else 1 for axis in AXES}
    dma = pltpu.SemaphoreType.DMA
    return pl.pallas_call(
        functools.partial(kernel, counts),
        out_shape=pltpu.VMEM(x.shape, x.dtype),
        in_specs=[pl.BlockSpec(memory_space=pl.ANY)] * 4,
        out_specs=pl.BlockSpec(memory_space=pltpu.VMEM),
        scratch_shapes=[
            pltpu.VMEM((STEPS, planes + 2, rows + 2, depth + 2 * PAD, lanes), x.dtype),
            pltpu.VMEM((3, planes, rows, depth, lanes), x.dtype),
            pltpu.VMEM((pieces(rows, LOADS)[-1][1], depth, lanes), x.dtype),
            pltpu.SemaphoreType.REGULAR((2,)),
            dma((max(len(pieces(rows, LOADS)), len(pieces(rows, CUTS[0]))),)),
            dma(()),
            dma((ways["py"], 2)),
            dma((ways["py"], most(rows, 0))),
            dma((ways["py"], most(rows, 1))),
            dma((ways["px"],)),
            dma((ways["px"], 2)),
            dma((ways["pz"],)),
            dma((ways["pz"], 2)),
            dma(()),
            dma(()),
        ],
        compiler_params=pltpu.CompilerParams(
            collective_id=0, has_side_effects=True, vmem_limit_bytes=54 * 2**20
        ),
    )(x, vn, ve, vu)


def solution(mesh):
    counts = {axis: mesh.shape[axis] for axis in (*AXES, "site")}
    spec = P(("site", "py"), "px", "pz", None)
    return jax.shard_map(
        functools.partial(body, counts), mesh=mesh, in_specs=(spec,) * 4, out_specs=spec,
        check_vma=False,
    )
```
